256 devices in a mesh: rows: 64 (over z, x, core), cols: 4 (over y).
Axes of the slice: x: 4, y: 4, z: 8, core: 2. Of those that a mesh axis runs over, the one named last changes fastest.
Arguments:
- source: float32 [8192, 32768], P('rows', 'cols'), may hold values from -6 to 6
- low_row: int32 [8192], replicated, may hold values from 0 to 8190, as said below
- weight_low: float32 [8192], replicated, may hold values from 0 to 1
Outputs:
- mercator: float32 [8192, 32768], P('rows', 'cols')
- level1: float32 [4096, 16384], P('rows', 'cols')
- level2: float32 [2048, 8192], P('rows', 'cols')
- level3: float32 [1024, 4096], P(('rows', 'cols'))
- level4: float32 [512, 2048], P(('rows', 'cols'))
The draws below stay inside these ranges and needn't reach their ends.
Inputs may be any that keep to these rules, and one draw needn't show every extreme that they name: With t = 68 degrees in radians, E = ln tan(pi/4 + t/2), y = E * (1 - (2m + 1) / 16384) and lat = 2 atan(exp(y)) - pi/2, the base row of Mercator row m is floor((t - lat) / t * 8192 - 0.5) clipped to the range; low_row[m] differs from it by at most 2 and is then clipped to the range.
All inputs are finite; a program needn't handle non-finite values.
Results may differ from the reference program's by a relative error of at most 0.00007.
Values sent between devices are 32-bit elements; how exact they have to be, the bound alone decides.
A program may use at most 128 MiB of HBM per device.

```python
import math
import jax
import jax.numpy as jnp

TOTAL = 8192
COLS = 32768


def draw_low_row(key, part):
    window_top = 68.0 * math.pi / 180.0
    north_edge = math.log(math.tan(math.pi / 4 + window_top / 2))
    centres = (2.0 * jnp.arange(TOTAL, dtype=jnp.float32) + 1.0) / (2.0 * TOTAL)
    merc_y = north_edge * (1.0 - centres)
    latitude = 2.0 * jnp.arctan(jnp.exp(merc_y)) - math.pi / 2
    position = (window_top - latitude) / window_top * TOTAL - 0.5
    base_rows = jnp.clip(jnp.floor(position), 0, TOTAL - 2).astype(jnp.int32)
    jitter = jax.random.randint(key, (TOTAL,), -2, 3, dtype=jnp.int32)
    return jnp.clip(base_rows + jitter, 0, TOTAL - 2).astype(jnp.int32)


def shard_levels(rng, extent, shards, low, high):
    def one(axis_at, shards_of):
        draws = jax.random.uniform(jax.random.fold_in(jax.random.fold_in(rng, 6), axis_at), (shards_of,), jnp.float32, low / len(shards), high / len(shards))
        return jnp.repeat(jnp.exp(draws), extent[axis_at] // shards_of).reshape((-1,) + (1,) * (len(extent) - axis_at - 1))

    loudness = one(*shards[0])
    for cut in shards[1:]:
        loudness = loudness * one(*cut)
    return loudness


def normal_values(key, dims, width, reach, split=(), kind=jnp.bfloat16):
    entries = width * jax.random.normal(key, dims, jnp.float32)
    if split:
        entries = entries * shard_levels(key, dims, split, -0.22, 0.18)
    return jnp.clip(entries, -reach, reach).astype(kind)


def setup_inputs(seed: int = 0) -> dict:
    arg_keys = jax.random.split(jax.random.key(seed), 4)
    return {
        "source": normal_values(arg_keys[0], (TOTAL, COLS), 1.0, 6.0, ((0, 64), (1, 4)), jnp.float32),
        "low_row": draw_low_row(jax.random.fold_in(arg_keys[3], 71), 0),
        "weight_low": jnp.clip(jax.random.uniform(arg_keys[2], (TOTAL,), jnp.float32, 0.0, 1.0), 0.0, 1.0),
    }


def blend(columns, low_row, weight_low):
    upper_rows = jnp.take(columns, low_row, axis=0)
    lower_rows = jnp.take(columns, low_row + 1, axis=0)
    scales = weight_low.reshape((-1,) + (1,) * (columns.ndim - 1))
    return scales * upper_rows + (1.0 - scales) * lower_rows


def halve(picture):
    return (picture[0::2, 0::2] + picture[1::2, 0::2] + picture[0::2, 1::2] + picture[1::2, 1::2]) * 0.25


def reference(source, low_row, weight_low):
    mercator = blend(source, low_row, weight_low)
    level1 = halve(mercator)
    level2 = halve(level1)
    level3 = halve(level2)
    level4 = halve(level3)
    return (mercator, level1, level2, level3, level4)
```

```python
import functools
import math

import jax
import jax.numpy as jnp
import numpy as np
from jax import lax
from jax.experimental import pallas as pl
from jax.experimental.pallas import tpu as pltpu
from jax.sharding import PartitionSpec as P

TOTAL = 8192
WIDTH = 8192
LINES = 128
DEVICES = 64
FIRST_BLENDED = 36
FIRST_KEPT = 61
CHUNKS = 4
CHUNK = WIDTH // CHUNKS
STEP = 1024

ROUTES = (
    ((2, 0, 4), 3),
    ((3, 0, 5), 11),
    ((5, 6, 7), 1),
    ((5, 4, 8), 21),
    ((6, 5, 9), 11),
    ((6, 26, 14, 10), 2),
    ((7, 4, 10), 3),
    ((7, 27, 15, 11), 7),
    ((8, 28, 16, 12), 2),
    ((9, 28, 16, 12), 5),
    ((9, 29, 17, 13), 4),
    ((10, 30, 17, 13), 3),
    ((10, 30, 18, 14), 6),
    ((11, 31, 19, 14), 2),
    ((11, 31, 19, 15), 9),
    ((12, 0, 20, 16), 7),
    ((13, 1, 21, 17), 9),
    ((14, 1, 21, 17), 4),
    ((14, 2, 22, 18), 2),
    ((15, 2, 22, 18), 7),
    ((17, 16, 20), 2),
    ((17, 4, 24, 20), 2),
    ((18, 6, 26, 22), 5),
    ((19, 16, 22), 4),
    ((19, 4, 24, 22), 1),
    ((20, 22, 23), 1),
    ((20, 27, 23), 2),
    ((21, 22, 23), 7),
    ((21, 20, 24), 12),
    ((22, 20, 24), 5),
    ((22, 21, 25), 1),
    ((23, 21, 25), 1),
    ((23, 24, 25), 5),
    ((23, 29, 25), 2),
    ((24, 27, 26), 7),
    ((25, 31, 27), 5),
    ((27, 24, 28), 9),
    ((28, 1, 29), 1),
)

RECEIVED = 20
OWN, MADE, TAKEN = 0, 16, 32
PASSED = TAKEN + RECEIVED


def row_range():
    top = 68.0 * math.pi / 180.0
    edge = math.log(math.tan(math.pi / 4 + top / 2))
    rows = np.arange(TOTAL)
    lat = 2.0 * np.arctan(np.exp(edge * (1.0 - (2 * rows + 1) / (2.0 * TOTAL)))) - math.pi / 2
    place = (top - lat) / top * TOTAL - 0.5
    first = np.clip(np.floor(place - 0.05), 0, TOTAL - 2).astype(int)
    last = np.clip(np.floor(place + 0.05), 0, TOTAL - 2).astype(int)
    return np.clip(first - 2, 0, TOTAL - 2), np.clip(last + 2, 0, TOTAL - 2) + 1


@functools.cache
def make_plan():
    low, high = row_range()
    flows = []
    head = [dict(sends=[], relays=[], locals=[], peers=set()) for _ in range(DEVICES)]
    made_first = {}
    for d in range(FIRST_BLENDED, DEVICES):
        for q in range(16 * d, 16 * d + 16):
            for s in range(low[8 * q] // LINES, min(high[8 * q + 7] // LINES, d - 1) + 1):
                made_first[s] = min(made_first.get(s, q), q)
    for r, h in enumerate(head):
        h["made_first"] = made_first.get(r, 0)
        h["made"] = 0
        h["extra"] = []
        h["used"] = [False] * RECEIVED
    for d in range(DEVICES):
        h = head[d]
        if d < FIRST_BLENDED:
            first, last = low[LINES * d] // 8, high[LINES * d + LINES - 1] // 8
            h["base"] = 8 * first
            h["count"] = last - first + 1
            for g in range(first, last + 1):
                flows.append((g // 16, d, OWN + g % 16, TAKEN + g - first))
        else:
            h["base"] = LINES * d
            for q in range(16 * d, 16 * d + 16):
                for n, s in enumerate(range(low[8 * q] // LINES, high[8 * q + 7] // LINES + 1)):
                    if s == d:
                        continue
                    place = q - made_first[s]
                    head[s]["made"] = max(head[s]["made"], place + 1)
                    if n == 0:
                        slot = q - 16 * d
                    else:
                        slot = 16 + len(h["extra"])
                        h["extra"].append(q - 16 * d)
                    flows.append((s, d, MADE + place, TAKEN + slot))
            h["count"] = 16 + len(h["extra"])
    routes = {}
    for way, blocks in ROUTES:
        routes.setdefault((way[0], way[-1]), []).extend([way] * blocks)
    passed = [0] * DEVICES
    for s, d, slot, goal in flows:
        head[d]["used"][goal - TAKEN] = True
        if s == d:
            head[s]["locals"].append((slot, goal))
            continue
        waiting = routes.get((s // 2, d // 2), [])
        way = waiting.pop() if waiting else (s // 2, d // 2)
        stops = []
        for chip in way[1:-1]:
            stop = min((2 * chip + s % 2, 2 * chip + 1 - s % 2), key=lambda v: passed[v])
            stops.append((stop, PASSED + passed[stop]))
            passed[stop] += 1
        stops.append((d, goal))
        at = s
        for leg, (stop, place) in enumerate(stops):
            if leg == 0:
                head[s]["sends"].append((-len(stops), slot, stop, place))
            else:
                head[at]["relays"].append((leg, -len(stops), slot, stop, place))
            head[at]["peers"].add(stop)
            head[stop]["peers"].add(at)
            at, slot = stop, place
    assert not any(routes.values())
    for h in head:
        inner = [i for i in range(16) if h["used"][i]]
        outer = [i for i in range(16, RECEIVED) if h["used"][i]]
        h["spans"] = []
        for some in (inner, outer):
            h["spans"] += [some[0], some[-1] + 1] if some else [0, 0]
            assert not some or len(some) == some[-1] + 1 - some[0]
        h["sends"] = [v[1:] for v in sorted(h["sends"], key=lambda v: v[0])]
        relays = sorted(h["relays"])
        h["early"] = sum(v[0] == 1 for v in relays)
        h["relays"] = [v[2:] for v in relays]
        h["peers"] = sorted(h["peers"])
    return head, max(passed)


(SENDS, EARLY, RELAYS, LOCALS, COUNT, MADE_COUNT, MADE_FIRST, BASE, EXTRAS, PEERS) = range(10)
SPANS, LISTS = 10, 14


def make_tables():
    head, most_passed = make_plan()
    width = lambda name: max(len(h[name]) for h in head)
    starts, at = {}, LISTS
    for name in ("extra", "peers", "locals", "sends", "relays"):
        starts[name] = at
        at += width(name) * (3 if name in ("locals", "sends", "relays") else 1)
    words = []
    for h in head:
        w = [None] * at
        w[SENDS], w[EARLY], w[RELAYS] = len(h["sends"]), h["early"], len(h["relays"])
        w[LOCALS], w[COUNT] = len(h["locals"]), int(h["count"])
        w[MADE_COUNT], w[MADE_FIRST] = int(h["made"]), int(h["made_first"])
        w[BASE], w[EXTRAS], w[PEERS] = int(h["base"]), len(h["extra"]), len(h["peers"])
        w[SPANS : SPANS + 4] = [int(v) for v in h["spans"]]
        for name in ("extra", "peers"):
            for i, v in enumerate(h[name]):
                w[starts[name] + i] = int(v)
        for i, (slot, place) in enumerate(h["locals"]):
            w[starts["locals"] + 3 * i : starts["locals"] + 3 * i + 3] = [int(slot), 0, int(place)]
        for name in ("sends", "relays"):
            for i, v in enumerate(h[name]):
                w[starts[name] + 3 * i : starts[name] + 3 * i + 3] = [int(x) for x in v]
        words.append(w)
    return words, starts, at, most_passed, width("sends"), width("relays")


def split(x):
    high = x.astype(jnp.bfloat16)
    return high, (x - high.astype(jnp.float32)).astype(jnp.bfloat16)


def mm(a, b):
    return jnp.dot(a, b, preferred_element_type=jnp.float32)


def weighted(weights, x):
    high, low = split(x)
    both = mm(weights, high)
    return both[:LINES] + both[LINES:] + mm(weights[:LINES], low)


def turned(row):
    return jnp.transpose(jnp.broadcast_to(row, (LINES, LINES)))


def kernel(
    words, starts, n_sends, most_extra,
    src, low_ref, weight_ref,
    merc, out1, out2, out3, out4,
    buf, tab, w_made, w_take, pool, tiles0, tiles1, tiles2, l3_send, l3_take,
    load_sem, send_sem, take_sem, y_send_sem, y_take_sem,
):
    r = lax.axis_index("rows")
    c = lax.axis_index("cols")

    def fill(low_half, count):
        if count == 1:
            for i, v in enumerate(words[low_half]):
                if v is not None:
                    tab[i] = v
            return
        half = count // 2
        lax.cond(
            r < low_half + half,
            lambda: fill(low_half, half),
            lambda: fill(low_half + half, half),
        )

    fill(0, DEVICES)

    def chunk(q):
        return pl.ds(q * CHUNK, CHUNK)

    loads = [
        pltpu.make_async_copy(
            src.at[:, :, chunk(q)], buf.at[q, pl.ds(OWN, 16)], load_sem.at[q]
        )
        for q in range(CHUNKS)
    ]
    for load in loads:
        load.start()

    barrier = pltpu.get_barrier_semaphore()
    n_peers = tab[PEERS]

    @pl.loop(0, n_peers)
    def _(i):
        pl.semaphore_signal(
            barrier, 1, device_id=(tab[starts["peers"] + i], c),
            device_id_type=pl.DeviceIdType.MESH,
        )

    for k in range(1, 4):
        pl.semaphore_signal(
            barrier, 1, device_id=(r, lax.rem(c + k, 4)), device_id_type=pl.DeviceIdType.MESH
        )

    n_made = tab[MADE_COUNT]

    @pl.when(n_made > 0)
    def _():
        first = tab[MADE_FIRST] * 8
        line, shift = first // LINES, lax.rem(first, LINES)
        after = jnp.minimum(line + 1, DEVICES - 1)
        lane = lax.broadcasted_iota(jnp.int32, (1, LINES), 1)

        def aligned(ref):
            one = pltpu.roll(jnp.broadcast_to(ref[pl.ds(line, 1), :], (8, LINES)), LINES - shift, 1)
            two = pltpu.roll(jnp.broadcast_to(ref[pl.ds(after, 1), :], (8, LINES)), LINES - shift, 1)
            return jnp.where(lane < LINES - shift, one[:1], two[:1])

        row = turned(aligned(low_ref))
        weight = turned(aligned(weight_ref))
        column = r * LINES + lax.broadcasted_iota(jnp.int32, (LINES, LINES), 1)
        values = jnp.where(row == column, weight, 0.0) + jnp.where(row + 1 == column, 1.0 - weight, 0.0)
        w_made[pl.ds(0, LINES), :], w_made[pl.ds(LINES, LINES), :] = split(values)

    pl.semaphore_wait(barrier, n_peers + 3)

    def copy(j, at, q):
        slot, device, place = tab[at], tab[at + 1], tab[at + 2]
        return pltpu.make_async_remote_copy(
            src_ref=buf.at[q, slot],
            dst_ref=buf.at[q, place],
            send_sem=send_sem.at[j, q],
            recv_sem=take_sem.at[place - TAKEN, q],
            device_id=(device, c),
            device_id_type=pl.DeviceIdType.MESH,
        )

    def arrived(place, q):
        return pltpu.make_async_remote_copy(
            src_ref=buf.at[q, place],
            dst_ref=buf.at[q, place],
            send_sem=send_sem.at[0, q],
            recv_sem=take_sem.at[place - TAKEN, q],
            device_id=(r, lax.rem(c + 1, 4)),
            device_id_type=pl.DeviceIdType.MESH,
        )

    n_own, n_locals = tab[SENDS], tab[LOCALS]
    for q in range(CHUNKS):
        loads[q].wait()

        @pl.when(n_made > 0)
        def _():
            @pl.loop(0, CHUNK // STEP)
            def _(t):
                columns = pl.ds(pl.multiple_of(t * STEP, STEP), STEP)
                x = buf[q, pl.ds(OWN, 16), :, columns].reshape(LINES, STEP)
                made = weighted(w_made[...], x)
                buf[q, pl.ds(MADE, 16), :, columns] = made.reshape(16, 8, STEP)

        @pl.loop(0, n_own)
        def _(j):
            copy(j, starts["sends"] + 3 * j, q).start()

        @pl.loop(0, n_locals)
        def _(i):
            place = tab[starts["locals"] + 3 * i + 2]
            pltpu.make_async_copy(
                src.at[tab[starts["locals"] + 3 * i], :, chunk(q)],
                buf.at[q, place],
                take_sem.at[place - TAKEN, q],
            ).start()

    blended = r >= FIRST_BLENDED
    n_taken = tab[COUNT]
    a = lax.broadcasted_iota(jnp.int32, (256, 128), 0)
    b = lax.broadcasted_iota(jnp.int32, (256, 128), 1)
    pool[...] = jnp.where(a // 2 == b, 0.25, 0.0).astype(jnp.bfloat16)

    @pl.when(jnp.logical_or(r < FIRST_BLENDED, r >= FIRST_KEPT))
    def _():
        row = turned(low_ref[pl.ds(r, 1), :]) - tab[BASE]
        weight = turned(weight_ref[pl.ds(r, 1), :])
        row = jnp.concatenate([row, row], axis=1)
        weight = jnp.concatenate([weight, weight], axis=1)
        column = lax.broadcasted_iota(jnp.int32, (LINES, 2 * LINES), 1)
        values = jnp.where(row == column, weight, 0.0) + jnp.where(row + 1 == column, 1.0 - weight, 0.0)
        high, low = split(values[:, : 8 * RECEIVED])
        w_take[pl.ds(0, LINES), :] = high
        w_take[pl.ds(LINES, LINES), :] = low

    n_early, n_relays = tab[EARLY], tab[RELAYS]

    def forward(j, q):
        at = starts["relays"] + 3 * j
        arrived(tab[at], q).wait_recv()
        copy(n_sends + j, at, q).start()

    for q in range(CHUNKS + 1):
        if q < CHUNKS:
            @pl.loop(0, n_early)
            def _(j):
                forward(j, q)
        if q > 0:
            @pl.loop(n_early, n_relays)
            def _(j):
                forward(j, q - 1)

    def pool_columns(blocks):
        rows = blocks[0].shape[0]
        high, low = split(jnp.concatenate(blocks, axis=0))
        both = mm(high, pool[...]) + mm(low, pool[...])
        return [both[rows * i : rows * i + rows] for i in range(len(blocks))]

    def halve(tiles, count, rows):
        def one(i):
            return tiles[i, pl.ds(0, rows, 2), :] + tiles[i, pl.ds(1, rows, 2), :]

        return pool_columns(
            [jnp.concatenate([one(i), one(i + 1)], axis=1) for i in range(0, count, 2)]
        )

    for q in range(CHUNKS):
        for span in (SPANS, SPANS + 2):
            @pl.loop(tab[span], tab[span + 1])
            def _(i):
                arrived(TAKEN + i, q).wait_recv()

        @pl.when(jnp.logical_not(blended))
        def _():
            for t in range(0, CHUNK, STEP):
                x = buf[q, pl.ds(TAKEN, RECEIVED), :, pl.ds(t, STEP)].reshape(8 * RECEIVED, STEP)
                x = jnp.where(lax.broadcasted_iota(jnp.int32, x.shape, 0) < 8 * n_taken, x, 0.0)
                merc[:, pl.ds(q * CHUNK + t, STEP)] = weighted(w_take[...], x)

        @pl.when(blended)
        def _():
            @pl.when(r < FIRST_KEPT)
            def _():
                merc[:, chunk(q)] = buf[q, pl.ds(TAKEN, 16)].reshape(LINES, CHUNK)

            @pl.when(r >= FIRST_KEPT)
            def _():
                for t in range(0, CHUNK, STEP):
                    x = buf[q, pl.ds(TAKEN, 16), :, pl.ds(t, STEP)].reshape(LINES, STEP)
                    x = jnp.where(lax.broadcasted_iota(jnp.int32, x.shape, 0) < 8 * tab[SPANS + 1], x, 0.0)
                    own = buf[q, pl.ds(OWN, 16), :, pl.ds(t, STEP)].reshape(LINES, STEP)
                    merc[:, pl.ds(q * CHUNK + t, STEP)] = x + weighted(w_take[:, :LINES], own)

            for i in range(most_extra):
                @pl.when(i < tab[EXTRAS])
                def _():
                    rows = pl.ds(pl.multiple_of(tab[starts["extra"] + i] * 8, 8), 8)
                    merc[rows, chunk(q)] += buf[q, TAKEN + 16 + i]

        for i in range(CHUNK // 128):
            tiles0[i] = merc[:, pl.ds(q * CHUNK + 128 * i, 128)]
        for i, part in enumerate(halve(tiles0, CHUNK // 128, 64)):
            tiles1[i] = part
            out1[:, pl.ds(q * CHUNK // 2 + 128 * i, 128)] = part
        for i, part in enumerate(halve(tiles1, CHUNK // 256, 32)):
            tiles2[i] = part
            out2[:, pl.ds(q * CHUNK // 4 + 128 * i, 128)] = part
        for i, part in enumerate(halve(tiles2, CHUNK // 512, 16)):
            for k in range(4):
                l3_send[k, :, pl.ds(q * CHUNK // 8 + 128 * i, 128)] = part[4 * k : 4 * k + 4]

    ys = []
    for k in range(1, 4):
        other = lax.rem(c + k, 4)
        ys.append(
            pltpu.make_async_remote_copy(
                src_ref=l3_send.at[other],
                dst_ref=l3_take.at[c],
                send_sem=y_send_sem.at[k - 1],
                recv_sem=y_take_sem.at[k - 1],
                device_id=(r, other),
                device_id_type=pl.DeviceIdType.MESH,
            )
        )
    for y in ys:
        y.start()
    for y in ys:
        y.wait_recv()
    for k in range(4):
        out3[:, pl.ds(k * WIDTH // 8, WIDTH // 8)] = jnp.where(c == k, l3_send[k], l3_take[k])
    level3 = out3[...]
    sums = jnp.concatenate(
        [level3[0:1] + level3[1:2], level3[2:3] + level3[3:4], jnp.zeros((6, WIDTH // 2), jnp.float32)],
        axis=0,
    )
    for i, part in enumerate(pool_columns([sums[:, 256 * i : 256 * i + 256] for i in range(16)])):
        out4[:, pl.ds(128 * i, 128)] = part[:2]

    for y in ys:
        y.wait_send()
    for q in range(CHUNKS):
        @pl.loop(0, n_own)
        def _(j):
            copy(j, starts["sends"] + 3 * j, q).wait_send()

        @pl.loop(0, n_relays)
        def _(j):
            copy(n_sends + j, starts["relays"] + 3 * j, q).wait_send()


def body(source, low_row, weight_low):
    words, starts, size, most_passed, n_sends, n_relays = make_tables()
    slots = PASSED + most_passed
    f32 = jnp.float32
    vmem = pl.BlockSpec(memory_space=pltpu.VMEM)
    return pl.pallas_call(
        functools.partial(kernel, words, starts, n_sends, starts["peers"] - starts["extra"]),
        out_shape=(
            jax.ShapeDtypeStruct((128, 8192), f32),
            jax.ShapeDtypeStruct((64, 4096), f32),
            jax.ShapeDtypeStruct((32, 2048), f32),
            jax.ShapeDtypeStruct((4, 4096), f32),
            jax.ShapeDtypeStruct((2, 2048), f32),
        ),
        in_specs=[pl.BlockSpec(memory_space=pl.ANY), vmem, vmem],
        out_specs=(vmem,) * 5,
        scratch_shapes=[
            pltpu.VMEM((CHUNKS, slots, 8, CHUNK), f32),
            pltpu.SMEM((size,), jnp.int32),
            pltpu.VMEM((2 * LINES, LINES), jnp.bfloat16),
            pltpu.VMEM((2 * LINES, 8 * RECEIVED), jnp.bfloat16),
            pltpu.VMEM((256, 128), jnp.bfloat16),
            pltpu.VMEM((CHUNK // 128, 128, 128), f32),
            pltpu.VMEM((CHUNK // 256, 64, 128), f32),
            pltpu.VMEM((CHUNK // 512, 32, 128), f32),
            pltpu.VMEM((4, 4, WIDTH // 8), f32),
            pltpu.VMEM((4, 4, WIDTH // 8), f32),
            pltpu.SemaphoreType.DMA((CHUNKS,)),
            pltpu.SemaphoreType.DMA((n_sends + n_relays, CHUNKS)),
            pltpu.SemaphoreType.DMA((RECEIVED + most_passed, CHUNKS)),
            pltpu.SemaphoreType.DMA((3,)),
            pltpu.SemaphoreType.DMA((3,)),
        ],
        compiler_params=pltpu.CompilerParams(
            collective_id=0, has_side_effects=True, vmem_limit_bytes=48 * 2**20
        ),
    )(source.reshape(16, 8, WIDTH), low_row.reshape(64, 128), weight_low.reshape(64, 128))


def solution(mesh):
    placed = (P("rows", "cols"), P(), P())
    return jax.shard_map(
        body,
        mesh=mesh,
        in_specs=placed,
        out_specs=(
            P("rows", "cols"),
            P("rows", "cols"),
            P("rows", "cols"),
            P(("rows", "cols"), None),
            P(("rows", "cols"), None),
        ),
        check_vma=False,
    )
```

```python
import functools
import math

import jax
import jax.numpy as jnp
import numpy as np
from jax import lax
from jax.experimental import pallas as pl
from jax.experimental.pallas import tpu as pltpu
from jax.sharding import PartitionSpec as P

TOTAL = 8192
WIDTH = 8192
LINES = 128
DEVICES = 64
FIRST_BLENDED = 36
FIRST_KEPT = 61
CHUNKS = 4
CHUNK = WIDTH // CHUNKS
STEP = 1024

ROUTES = (
    ((2, 0, 4), 2),
    ((3, 0, 5), 11),
    ((5, 4, 8), 21),
    ((6, 5, 9), 12),
    ((7, 4, 10), 4),
    ((7, 27, 15, 11), 5),
    ((8, 28, 16, 12), 1),
    ((9, 28, 16, 12), 5),
    ((9, 29, 17, 13), 3),
    ((10, 30, 17, 13), 3),
    ((10, 30, 18, 14), 5),
    ((11, 31, 19, 14), 2),
    ((11, 31, 19, 15), 8),
    ((12, 0, 20, 16), 6),
    ((13, 1, 21, 17), 8),
    ((14, 2, 22, 17), 5),
    ((15, 2, 22, 18), 6),
    ((17, 16, 20), 5),
    ((18, 17, 21), 2),
    ((18, 6, 26, 22), 2),
    ((19, 16, 22), 2),
    ((19, 6, 26, 22), 1),
    ((19, 7, 27, 23), 1),
    ((20, 27, 23), 2),
    ((21, 22, 23), 7),
    ((21, 20, 24), 14),
    ((22, 20, 24), 4),
    ((22, 21, 25), 3),
    ((23, 24, 25), 5),
    ((24, 22, 26), 1),
    ((24, 27, 26), 5),
    ((25, 31, 27), 2),
    ((27, 24, 28), 8),
)

RECEIVED = 20
OWN, MADE, TAKEN = 0, 16, 32
PASSED = TAKEN + RECEIVED


def row_range():
    top = 68.0 * math.pi / 180.0
    edge = math.log(math.tan(math.pi / 4 + top / 2))
    rows = np.arange(TOTAL)
    lat = 2.0 * np.arctan(np.exp(edge * (1.0 - (2 * rows + 1) / (2.0 * TOTAL)))) - math.pi / 2
    place = (top - lat) / top * TOTAL - 0.5
    first = np.clip(np.floor(place - 0.05), 0, TOTAL - 2).astype(int)
    last = np.clip(np.floor(place + 0.05), 0, TOTAL - 2).astype(int)
    return np.clip(first - 2, 0, TOTAL - 2), np.clip(last + 2, 0, TOTAL - 2) + 1


@functools.cache
def make_plan():
    low, high = row_range()
    flows = []
    head = [dict(sends=[], relays=[], locals=[], peers=set()) for _ in range(DEVICES)]
    made_first = {}
    for d in range(FIRST_BLENDED, DEVICES):
        for q in range(16 * d, 16 * d + 16):
            for s in range(low[8 * q] // LINES, min(high[8 * q + 7] // LINES, d - 1) + 1):
                made_first[s] = min(made_first.get(s, q), q)
    for r, h in enumerate(head):
        h["made_first"] = made_first.get(r, 0)
        h["made"] = 0
        h["extra"] = []
        h["used"] = [False] * RECEIVED
    for d in range(DEVICES):
        h = head[d]
        if d < FIRST_BLENDED:
            first, last = low[LINES * d] // 8, high[LINES * d + LINES - 1] // 8
            h["base"] = 8 * first
            h["count"] = last - first + 1
            for g in range(first, last + 1):
                flows.append((g // 16, d, OWN + g % 16, TAKEN + g - first))
        else:
            h["base"] = LINES * d
            for q in range(16 * d, 16 * d + 16):
                for n, s in enumerate(range(low[8 * q] // LINES, high[8 * q + 7] // LINES + 1)):
                    if s == d:
                        continue
                    place = q - made_first[s]
                    head[s]["made"] = max(head[s]["made"], place + 1)
                    if n == 0:
                        slot = q - 16 * d
                    else:
                        slot = 16 + len(h["extra"])
                        h["extra"].append(q - 16 * d)
                    flows.append((s, d, MADE + place, TAKEN + slot))
            h["count"] = 16 + len(h["extra"])
    between = {}
    for s, d, _, _ in flows:
        between[s // 2, d // 2] = between.get((s // 2, d // 2), 0) + 1
    ways = {}
    for way, blocks in ROUTES:
        ways.setdefault((way[0], way[-1]), []).append([blocks, way])
    routes = {}
    for pair, total in between.items():
        counts = ways.get(pair, [])
        rest = total - sum(n for n, _ in counts)
        assert rest >= 0
        marks = [((i + 0.5) / n, way) for n, way in counts + [[rest, pair]] for i in range(n)]
        routes[pair] = [way for _, way in sorted(marks)]
    passed = [0] * DEVICES
    for s, d, slot, goal in flows:
        head[d]["used"][goal - TAKEN] = True
        if s == d:
            head[s]["locals"].append((slot, goal))
            routes[s // 2, d // 2].pop()
            continue
        way = routes[s // 2, d // 2].pop()
        stops = []
        for chip in way[1:-1]:
            stop = min((2 * chip + s % 2, 2 * chip + 1 - s % 2), key=lambda v: passed[v])
            stops.append((stop, PASSED + passed[stop]))
            passed[stop] += 1
        stops.append((d, goal))
        at = s
        for leg, (stop, place) in enumerate(stops):
            if leg == 0:
                head[s]["sends"].append((-len(stops), slot, stop, place))
            else:
                head[at]["relays"].append((leg, -len(stops), slot, stop, place))
            head[at]["peers"].add(stop)
            head[stop]["peers"].add(at)
            at, slot = stop, place
    assert not any(routes.values())
    for h in head:
        inner = [i for i in range(16) if h["used"][i]]
        outer = [i for i in range(16, RECEIVED) if h["used"][i]]
        h["spans"] = []
        for some in (inner, outer):
            h["spans"] += [some[0], some[-1] + 1] if some else [0, 0]
            assert not some or len(some) == some[-1] + 1 - some[0]
        turns, seen = [], {}
        for stops, *move in sorted(h["sends"], key=lambda v: v[0]):
            key = stops, move[1]
            seen[key] = seen.get(key, 0) + 1
            turns.append((stops == -1, key, seen[key], move))
        h["sends"] = [
            move for _, _, _, move in sorted(turns, key=lambda v: (v[0], (v[2] - 0.5) / seen[v[1]], v[1]))
        ]
        relays = sorted(h["relays"])
        h["early"] = sum(v[0] == 1 for v in relays)
        h["relays"] = [v[2:] for v in relays]
        h["peers"] = sorted(h["peers"])
    return head, max(passed)


(SENDS, EARLY, RELAYS, LOCALS, COUNT, MADE_COUNT, MADE_FIRST, BASE, EXTRAS, PEERS) = range(10)
SPANS, LISTS = 10, 14


def make_tables():
    head, most_passed = make_plan()
    width = lambda name: max(len(h[name]) for h in head)
    starts, at = {}, LISTS
    for name in ("extra", "peers", "locals", "sends", "relays"):
        starts[name] = at
        at += width(name) * (3 if name in ("locals", "sends", "relays") else 1)
    words = []
    for h in head:
        w = [None] * at
        w[SENDS], w[EARLY], w[RELAYS] = len(h["sends"]), h["early"], len(h["relays"])
        w[LOCALS], w[COUNT] = len(h["locals"]), int(h["count"])
        w[MADE_COUNT], w[MADE_FIRST] = int(h["made"]), int(h["made_first"])
        w[BASE], w[EXTRAS], w[PEERS] = int(h["base"]), len(h["extra"]), len(h["peers"])
        w[SPANS : SPANS + 4] = [int(v) for v in h["spans"]]
        for name in ("extra", "peers"):
            for i, v in enumerate(h[name]):
                w[starts[name] + i] = int(v)
        for i, (slot, place) in enumerate(h["locals"]):
            w[starts["locals"] + 3 * i : starts["locals"] + 3 * i + 3] = [int(slot), 0, int(place)]
        for name in ("sends", "relays"):
            for i, v in enumerate(h[name]):
                w[starts[name] + 3 * i : starts[name] + 3 * i + 3] = [int(x) for x in v]
        words.append(w)
    return words, starts, at, most_passed, width("sends"), width("relays")


def split(x):
    high = x.astype(jnp.bfloat16)
    return high, (x - high.astype(jnp.float32)).astype(jnp.bfloat16)


def mm(a, b):
    return jnp.dot(a, b, preferred_element_type=jnp.float32)


def weighted(weights, x):
    high, low = split(x)
    both = mm(weights, high)
    return both[:LINES] + both[LINES:] + mm(weights[:LINES], low)


def turned(row):
    return jnp.transpose(jnp.broadcast_to(row, (LINES, LINES)))


def kernel(
    words, starts, n_sends, most_extra,
    src, low_ref, weight_ref,
    merc, out1, out2, out3, out4,
    buf, tab, w_made, w_take, pool, tiles0, tiles1, tiles2, l3_send, l3_take,
    load_sem, send_sem, take_sem, y_send_sem, y_take_sem,
):
    r = lax.axis_index("rows")
    c = lax.axis_index("cols")

    def fill(low_half, count):
        if count == 1:
            for i, v in enumerate(words[low_half]):
                if v is not None:
                    tab[i] = v
            return
        half = count // 2
        lax.cond(
            r < low_half + half,
            lambda: fill(low_half, half),
            lambda: fill(low_half + half, half),
        )

    fill(0, DEVICES)

    def chunk(q):
        return pl.ds(q * CHUNK, CHUNK)

    loads = [
        pltpu.make_async_copy(
            src.at[:, :, chunk(q)], buf.at[q, pl.ds(OWN, 16)], load_sem.at[q]
        )
        for q in range(CHUNKS)
    ]
    for load in loads:
        load.start()

    barrier = pltpu.get_barrier_semaphore()
    n_peers = tab[PEERS]

    @pl.loop(0, n_peers)
    def _(i):
        pl.semaphore_signal(
            barrier, 1, device_id=(tab[starts["peers"] + i], c),
            device_id_type=pl.DeviceIdType.MESH,
        )

    for k in range(1, 4):
        pl.semaphore_signal(
            barrier, 1, device_id=(r, lax.rem(c + k, 4)), device_id_type=pl.DeviceIdType.MESH
        )

    n_made = tab[MADE_COUNT]

    @pl.when(n_made > 0)
    def _():
        first = tab[MADE_FIRST] * 8
        line, shift = first // LINES, lax.rem(first, LINES)
        after = jnp.minimum(line + 1, DEVICES - 1)
        lane = lax.broadcasted_iota(jnp.int32, (1, LINES), 1)

        def aligned(ref):
            one = pltpu.roll(jnp.broadcast_to(ref[pl.ds(line, 1), :], (8, LINES)), LINES - shift, 1)
            two = pltpu.roll(jnp.broadcast_to(ref[pl.ds(after, 1), :], (8, LINES)), LINES - shift, 1)
            return jnp.where(lane < LINES - shift, one[:1], two[:1])

        row = turned(aligned(low_ref))
        weight = turned(aligned(weight_ref))
        column = r * LINES + lax.broadcasted_iota(jnp.int32, (LINES, LINES), 1)
        values = jnp.where(row == column, weight, 0.0) + jnp.where(row + 1 == column, 1.0 - weight, 0.0)
        w_made[pl.ds(0, LINES), :], w_made[pl.ds(LINES, LINES), :] = split(values)

    pl.semaphore_wait(barrier, n_peers + 3)

    def copy(j, at, q):
        slot, device, place = tab[at], tab[at + 1], tab[at + 2]
        return pltpu.make_async_remote_copy(
            src_ref=buf.at[q, slot],
            dst_ref=buf.at[q, place],
            send_sem=send_sem.at[j, q],
            recv_sem=take_sem.at[place - TAKEN, q],
            device_id=(device, c),
            device_id_type=pl.DeviceIdType.MESH,
        )

    def arrived(place, q):
        return pltpu.make_async_remote_copy(
            src_ref=buf.at[q, place],
            dst_ref=buf.at[q, place],
            send_sem=send_sem.at[0, q],
            recv_sem=take_sem.at[place - TAKEN, q],
            device_id=(r, lax.rem(c + 1, 4)),
            device_id_type=pl.DeviceIdType.MESH,
        )

    n_own, n_locals = tab[SENDS], tab[LOCALS]
    for q in range(CHUNKS):
        loads[q].wait()

        @pl.when(n_made > 0)
        def _():
            @pl.loop(0, CHUNK // STEP)
            def _(t):
                columns = pl.ds(pl.multiple_of(t * STEP, STEP), STEP)
                x = buf[q, pl.ds(OWN, 16), :, columns].reshape(LINES, STEP)
                made = weighted(w_made[...], x)
                buf[q, pl.ds(MADE, 16), :, columns] = made.reshape(16, 8, STEP)

        @pl.loop(0, n_own)
        def _(j):
            copy(j, starts["sends"] + 3 * j, q).start()

        @pl.loop(0, n_locals)
        def _(i):
            place = tab[starts["locals"] + 3 * i + 2]
            pltpu.make_async_copy(
                src.at[tab[starts["locals"] + 3 * i], :, chunk(q)],
                buf.at[q, place],
                take_sem.at[place - TAKEN, q],
            ).start()

    blended = r >= FIRST_BLENDED
    n_taken = tab[COUNT]
    a = lax.broadcasted_iota(jnp.int32, (256, 128), 0)
    b = lax.broadcasted_iota(jnp.int32, (256, 128), 1)
    pool[...] = jnp.where(a // 2 == b, 0.25, 0.0).astype(jnp.bfloat16)

    @pl.when(jnp.logical_or(r < FIRST_BLENDED, r >= FIRST_KEPT))
    def _():
        row = turned(low_ref[pl.ds(r, 1), :]) - tab[BASE]
        weight = turned(weight_ref[pl.ds(r, 1), :])
        row = jnp.concatenate([row, row], axis=1)
        weight = jnp.concatenate([weight, weight], axis=1)
        column = lax.broadcasted_iota(jnp.int32, (LINES, 2 * LINES), 1)
        values = jnp.where(row == column, weight, 0.0) + jnp.where(row + 1 == column, 1.0 - weight, 0.0)
        high, low = split(values[:, : 8 * RECEIVED])
        w_take[pl.ds(0, LINES), :] = high
        w_take[pl.ds(LINES, LINES), :] = low

    n_early, n_relays = tab[EARLY], tab[RELAYS]

    def forward(j, q):
        at = starts["relays"] + 3 * j
        arrived(tab[at], q).wait_recv()
        copy(n_sends + j, at, q).start()

    for q in range(CHUNKS + 1):
        if q < CHUNKS:
            @pl.loop(0, n_early)
            def _(j):
                forward(j, q)
        if q > 0:
            @pl.loop(n_early, n_relays)
            def _(j):
                forward(j, q - 1)

    def pool_columns(blocks):
        rows = blocks[0].shape[0]
        high, low = split(jnp.concatenate(blocks, axis=0))
        both = mm(high, pool[...]) + mm(low, pool[...])
        return [both[rows * i : rows * i + rows] for i in range(len(blocks))]

    def halve(tiles, count, rows):
        def one(i):
            return tiles[i, pl.ds(0, rows, 2), :] + tiles[i, pl.ds(1, rows, 2), :]

        return pool_columns(
            [jnp.concatenate([one(i), one(i + 1)], axis=1) for i in range(0, count, 2)]
        )

    for q in range(CHUNKS):
        for span in (SPANS, SPANS + 2):
            @pl.loop(tab[span], tab[span + 1])
            def _(i):
                arrived(TAKEN + i, q).wait_recv()

        @pl.when(jnp.logical_not(blended))
        def _():
            for t in range(0, CHUNK, STEP):
                x = buf[q, pl.ds(TAKEN, RECEIVED), :, pl.ds(t, STEP)].reshape(8 * RECEIVED, STEP)
                x = jnp.where(lax.broadcasted_iota(jnp.int32, x.shape, 0) < 8 * n_taken, x, 0.0)
                merc[:, pl.ds(q * CHUNK + t, STEP)] = weighted(w_take[...], x)

        @pl.when(blended)
        def _():
            @pl.when(r < FIRST_KEPT)
            def _():
                merc[:, chunk(q)] = buf[q, pl.ds(TAKEN, 16)].reshape(LINES, CHUNK)

            @pl.when(r >= FIRST_KEPT)
            def _():
                for t in range(0, CHUNK, STEP):
                    x = buf[q, pl.ds(TAKEN, 16), :, pl.ds(t, STEP)].reshape(LINES, STEP)
                    x = jnp.where(lax.broadcasted_iota(jnp.int32, x.shape, 0) < 8 * tab[SPANS + 1], x, 0.0)
                    own = buf[q, pl.ds(OWN, 16), :, pl.ds(t, STEP)].reshape(LINES, STEP)
                    merc[:, pl.ds(q * CHUNK + t, STEP)] = x + weighted(w_take[:, :LINES], own)

            for i in range(most_extra):
                @pl.when(i < tab[EXTRAS])
                def _():
                    rows = pl.ds(pl.multiple_of(tab[starts["extra"] + i] * 8, 8), 8)
                    merc[rows, chunk(q)] += buf[q, TAKEN + 16 + i]

        for i in range(CHUNK // 128):
            tiles0[i] = merc[:, pl.ds(q * CHUNK + 128 * i, 128)]
        for i, part in enumerate(halve(tiles0, CHUNK // 128, 64)):
            tiles1[i] = part
            out1[:, pl.ds(q * CHUNK // 2 + 128 * i, 128)] = part
        for i, part in enumerate(halve(tiles1, CHUNK // 256, 32)):
            tiles2[i] = part
            out2[:, pl.ds(q * CHUNK // 4 + 128 * i, 128)] = part
        for i, part in enumerate(halve(tiles2, CHUNK // 512, 16)):
            for k in range(4):
                l3_send[k, :, pl.ds(q * CHUNK // 8 + 128 * i, 128)] = part[4 * k : 4 * k + 4]

    ys = []
    for k in range(1, 4):
        other = lax.rem(c + k, 4)
        ys.append(
            pltpu.make_async_remote_copy(
                src_ref=l3_send.at[other],
                dst_ref=l3_take.at[c],
                send_sem=y_send_sem.at[k - 1],
                recv_sem=y_take_sem.at[k - 1],
                device_id=(r, other),
                device_id_type=pl.DeviceIdType.MESH,
            )
        )
    for y in ys:
        y.start()
    for y in ys:
        y.wait_recv()
    for k in range(4):
        out3[:, pl.ds(k * WIDTH // 8, WIDTH // 8)] = jnp.where(c == k, l3_send[k], l3_take[k])
    level3 = out3[...]
    sums = jnp.concatenate(
        [level3[0:1] + level3[1:2], level3[2:3] + level3[3:4], jnp.zeros((6, WIDTH // 2), jnp.float32)],
        axis=0,
    )
    for i, part in enumerate(pool_columns([sums[:, 256 * i : 256 * i + 256] for i in range(16)])):
        out4[:, pl.ds(128 * i, 128)] = part[:2]

    for y in ys:
        y.wait_send()
    for q in range(CHUNKS):
        @pl.loop(0, n_own)
        def _(j):
            copy(j, starts["sends"] + 3 * j, q).wait_send()

        @pl.loop(0, n_relays)
        def _(j):
            copy(n_sends + j, starts["relays"] + 3 * j, q).wait_send()


def store(*refs):
    *arrays, sems = refs
    copies = []
    for i in range(4):
        rows = pl.ds(32 * i, 32)
        copies.append(pltpu.make_async_copy(arrays[0].at[rows], arrays[5].at[rows], sems.at[i]))
    for i in range(1, 5):
        copies.append(pltpu.make_async_copy(arrays[i], arrays[5 + i], sems.at[3 + i]))
    for copy in copies:
        copy.start()
    for copy in copies:
        copy.wait()


def body(source, low_row, weight_low):
    words, starts, size, most_passed, n_sends, n_relays = make_tables()
    slots = PASSED + most_passed
    f32 = jnp.float32
    vmem = pl.BlockSpec(memory_space=pltpu.VMEM)
    results = pl.pallas_call(
        functools.partial(kernel, words, starts, n_sends, starts["peers"] - starts["extra"]),
        out_shape=(
            jax.ShapeDtypeStruct((128, 8192), f32),
            jax.ShapeDtypeStruct((64, 4096), f32),
            jax.ShapeDtypeStruct((32, 2048), f32),
            jax.ShapeDtypeStruct((4, 4096), f32),
            jax.ShapeDtypeStruct((2, 2048), f32),
        ),
        in_specs=[pl.BlockSpec(memory_space=pl.ANY), vmem, vmem],
        out_specs=(vmem,) * 5,
        scratch_shapes=[
            pltpu.VMEM((CHUNKS, slots, 8, CHUNK), f32),
            pltpu.SMEM((size,), jnp.int32),
            pltpu.VMEM((2 * LINES, LINES), jnp.bfloat16),
            pltpu.VMEM((2 * LINES, 8 * RECEIVED), jnp.bfloat16),
            pltpu.VMEM((256, 128), jnp.bfloat16),
            pltpu.VMEM((CHUNK // 128, 128, 128), f32),
            pltpu.VMEM((CHUNK // 256, 64, 128), f32),
            pltpu.VMEM((CHUNK // 512, 32, 128), f32),
            pltpu.VMEM((4, 4, WIDTH // 8), f32),
            pltpu.VMEM((4, 4, WIDTH // 8), f32),
            pltpu.SemaphoreType.DMA((CHUNKS,)),
            pltpu.SemaphoreType.DMA((n_sends + n_relays, CHUNKS)),
            pltpu.SemaphoreType.DMA((RECEIVED + most_passed, CHUNKS)),
            pltpu.SemaphoreType.DMA((3,)),
            pltpu.SemaphoreType.DMA((3,)),
        ],
        compiler_params=pltpu.CompilerParams(
            collective_id=0, has_side_effects=True, vmem_limit_bytes=48 * 2**20
        ),
    )(source.reshape(16, 8, WIDTH), low_row.reshape(64, 128), weight_low.reshape(64, 128))
    return pl.pallas_call(
        store,
        out_shape=tuple(jax.ShapeDtypeStruct(v.shape, v.dtype) for v in results),
        in_specs=[vmem] * 5,
        out_specs=(pl.BlockSpec(memory_space=pl.ANY),) * 5,
        scratch_shapes=[pltpu.SemaphoreType.DMA((8,))],
        compiler_params=pltpu.CompilerParams(vmem_limit_bytes=2**20),
    )(*results)


def solution(mesh):
    placed = (P("rows", "cols"), P(), P())
    return jax.shard_map(
        body,
        mesh=mesh,
        in_specs=placed,
        out_specs=(
            P("rows", "cols"),
            P("rows", "cols"),
            P("rows", "cols"),
            P(("rows", "cols"), None),
            P(("rows", "cols"), None),
        ),
        check_vma=False,
    )
```

```python
import functools
import math

import jax
import jax.numpy as jnp
import numpy as np
from jax import lax
from jax.experimental import pallas as pl
from jax.experimental.pallas import tpu as pltpu
from jax.sharding import PartitionSpec as P

TOTAL = 8192
WIDTH = 8192
LINES = 128
DEVICES = 64
FIRST_BLENDED = 36
FIRST_KEPT = 61
CHUNKS = 4
CHUNK = WIDTH // CHUNKS
STEP = 1024

ROUTES = (
    ((2, 5, 4), 1),
    ((3, 1, 5), 12),
    ((4, 3, 7), 1),
    ((5, 6, 7), 1),
    ((5, 4, 8), 17),
    ((6, 5, 9), 10),
    ((7, 4, 10), 1),
    ((7, 23, 10), 6),
    ((9, 8, 12), 1),
    ((9, 28, 12), 4),
    ((9, 29, 13), 1),
    ((10, 30, 14), 6),
    ((11, 31, 15), 8),
    ((12, 28, 16), 4),
    ((13, 28, 16), 3),
    ((13, 29, 17), 3),
    ((14, 30, 18), 3),
    ((15, 31, 19), 4),
    ((17, 16, 20), 2),
    ((18, 16, 21), 2),
    ((18, 17, 21), 1),
    ((19, 16, 22), 3),
    ((19, 18, 22), 1),
    ((19, 20, 22), 2),
    ((20, 19, 23), 2),
    ((20, 27, 23), 2),
    ((21, 22, 23), 7),
    ((21, 16, 24), 2),
    ((21, 20, 24), 9),
    ((22, 20, 24), 2),
    ((22, 23, 24), 4),
    ((23, 20, 25), 5),
    ((23, 29, 25), 5),
    ((24, 27, 26), 8),
    ((25, 31, 27), 7),
    ((27, 24, 28), 10),
    ((28, 31, 29), 2),
)

RECEIVED = 20
OWN, MADE, TAKEN = 0, 16, 32
PASSED = TAKEN + RECEIVED


def row_range():
    top = 68.0 * math.pi / 180.0
    edge = math.log(math.tan(math.pi / 4 + top / 2))
    rows = np.arange(TOTAL)
    lat = 2.0 * np.arctan(np.exp(edge * (1.0 - (2 * rows + 1) / (2.0 * TOTAL)))) - math.pi / 2
    place = (top - lat) / top * TOTAL - 0.5
    first = np.clip(np.floor(place - 0.05), 0, TOTAL - 2).astype(int)
    last = np.clip(np.floor(place + 0.05), 0, TOTAL - 2).astype(int)
    return np.clip(first - 2, 0, TOTAL - 2), np.clip(last + 2, 0, TOTAL - 2) + 1


@functools.cache
def make_plan():
    low, high = row_range()
    flows = []
    head = [dict(sends=[], relays=[], locals=[], peers=set()) for _ in range(DEVICES)]
    made_first = {}
    for d in range(FIRST_BLENDED, DEVICES):
        for q in range(16 * d, 16 * d + 16):
            for s in range(low[8 * q] // LINES, min(high[8 * q + 7] // LINES, d - 1) + 1):
                made_first[s] = min(made_first.get(s, q), q)
    for r, h in enumerate(head):
        h["made_first"] = made_first.get(r, 0)
        h["made"] = 0
        h["extra"] = []
        h["used"] = [False] * RECEIVED
    for d in range(DEVICES):
        h = head[d]
        if d < FIRST_BLENDED:
            first, last = low[LINES * d] // 8, high[LINES * d + LINES - 1] // 8
            h["base"] = 8 * first
            h["count"] = last - first + 1
            for g in range(first, last + 1):
                flows.append((g // 16, d, OWN + g % 16, TAKEN + g - first))
        else:
            h["base"] = LINES * d
            for q in range(16 * d, 16 * d + 16):
                for n, s in enumerate(range(low[8 * q] // LINES, high[8 * q + 7] // LINES + 1)):
                    if s == d:
                        continue
                    place = q - made_first[s]
                    head[s]["made"] = max(head[s]["made"], place + 1)
                    if n == 0:
                        slot = q - 16 * d
                    else:
                        slot = 16 + len(h["extra"])
                        h["extra"].append(q - 16 * d)
                    flows.append((s, d, MADE + place, TAKEN + slot))
            h["count"] = 16 + len(h["extra"])
    between = {}
    for s, d, _, _ in flows:
        between[s // 2, d // 2] = between.get((s // 2, d // 2), 0) + 1
    ways = {}
    for way, blocks in ROUTES:
        ways.setdefault((way[0], way[-1]), []).append([blocks, way])
    routes = {}
    for pair, total in between.items():
        counts = ways.get(pair, [])
        rest = total - sum(n for n, _ in counts)
        assert rest >= 0
        marks = [((i + 0.5) / n, way) for n, way in counts + [[rest, pair]] for i in range(n)]
        routes[pair] = [way for _, way in sorted(marks)]
    loads, sides = [0] * DEVICES, {}
    for way, blocks in sorted(ROUTES, key=lambda v: -v[1]):
        for chip in way[1:-1]:
            sides[way, chip] = int(loads[2 * chip + 1] < loads[2 * chip])
            loads[2 * chip + sides[way, chip]] += blocks
    passed = [0] * DEVICES
    for s, d, slot, goal in flows:
        head[d]["used"][goal - TAKEN] = True
        if s == d:
            head[s]["locals"].append((slot, goal))
            routes[s // 2, d // 2].pop()
            continue
        way = routes[s // 2, d // 2].pop()
        stops = []
        for chip in way[1:-1]:
            stop = 2 * chip + sides[way, chip]
            stops.append((stop, PASSED + passed[stop]))
            passed[stop] += 1
        stops.append((d, goal))
        at = s
        for leg, (stop, place) in enumerate(stops):
            if leg == 0:
                head[s]["sends"].append((-len(stops), slot, stop, place))
            else:
                head[at]["relays"].append((leg, -len(stops), slot, stop, place))
            head[at]["peers"].add(stop)
            head[stop]["peers"].add(at)
            at, slot = stop, place
    assert not any(routes.values())
    for h in head:
        inner = [i for i in range(16) if h["used"][i]]
        outer = [i for i in range(16, RECEIVED) if h["used"][i]]
        h["spans"] = []
        for some in (inner, outer):
            h["spans"] += [some[0], some[-1] + 1] if some else [0, 0]
            assert not some or len(some) == some[-1] + 1 - some[0]
        turns, seen = [], {}
        for stops, *move in sorted(h["sends"], key=lambda v: v[0]):
            key = stops, move[1]
            seen[key] = seen.get(key, 0) + 1
            turns.append((stops == -1, key, seen[key], move))
        h["sends"] = [
            move for _, _, _, move in sorted(turns, key=lambda v: (v[0], (v[2] - 0.5) / seen[v[1]], v[1]))
        ]
        relays = sorted(h["relays"])
        h["early"] = sum(v[0] == 1 for v in relays)
        h["relays"] = [v[2:] for v in relays]
        h["peers"] = sorted(h["peers"])
    return head, max(passed)


(SENDS, EARLY, RELAYS, LOCALS, COUNT, MADE_COUNT, MADE_FIRST, BASE, EXTRAS, PEERS) = range(10)
SPANS, LISTS = 10, 14


def make_tables():
    head, most_passed = make_plan()
    width = lambda name: max(len(h[name]) for h in head)
    starts, at = {}, LISTS
    for name in ("extra", "peers", "locals", "sends", "relays"):
        starts[name] = at
        at += width(name) * (3 if name in ("locals", "sends", "relays") else 1)
    words = []
    for h in head:
        w = [None] * at
        w[SENDS], w[EARLY], w[RELAYS] = len(h["sends"]), h["early"], len(h["relays"])
        w[LOCALS], w[COUNT] = len(h["locals"]), int(h["count"])
        w[MADE_COUNT], w[MADE_FIRST] = int(h["made"]), int(h["made_first"])
        w[BASE], w[EXTRAS], w[PEERS] = int(h["base"]), len(h["extra"]), len(h["peers"])
        w[SPANS : SPANS + 4] = [int(v) for v in h["spans"]]
        for name in ("extra", "peers"):
            for i, v in enumerate(h[name]):
                w[starts[name] + i] = int(v)
        for i, (slot, place) in enumerate(h["locals"]):
            w[starts["locals"] + 3 * i : starts["locals"] + 3 * i + 3] = [int(slot), 0, int(place)]
        for name in ("sends", "relays"):
            for i, v in enumerate(h[name]):
                w[starts[name] + 3 * i : starts[name] + 3 * i + 3] = [int(x) for x in v]
        words.append(w)
    return words, starts, at, most_passed, width("sends"), width("relays")


def split(x):
    high = x.astype(jnp.bfloat16)
    return high, (x - high.astype(jnp.float32)).astype(jnp.bfloat16)


def mm(a, b):
    return jnp.dot(a, b, preferred_element_type=jnp.float32)


def weighted(weights, x):
    high, low = split(x)
    both = mm(weights, high)
    return both[:LINES] + both[LINES:] + mm(weights[:LINES], low)


def turned(row):
    return jnp.transpose(jnp.broadcast_to(row, (LINES, LINES)))


def kernel(
    words, starts, n_sends, most_extra,
    src, low_ref, weight_ref,
    merc, out1, out2, out3, out4,
    buf, tab, w_made, w_take, pool, tiles0, tiles1, tiles2, l3_send, l3_take,
    load_sem, send_sem, take_sem, y_send_sem, y_take_sem,
):
    r = lax.axis_index("rows")
    c = lax.axis_index("cols")

    def fill(low_half, count):
        if count == 1:
            for i, v in enumerate(words[low_half]):
                if v is not None:
                    tab[i] = v
            return
        half = count // 2
        lax.cond(
            r < low_half + half,
            lambda: fill(low_half, half),
            lambda: fill(low_half + half, half),
        )

    fill(0, DEVICES)

    def chunk(q):
        return pl.ds(q * CHUNK, CHUNK)

    loads = [
        pltpu.make_async_copy(
            src.at[:, :, chunk(q)], buf.at[q, pl.ds(OWN, 16)], load_sem.at[q]
        )
        for q in range(CHUNKS)
    ]
    for load in loads:
        load.start()

    barrier = pltpu.get_barrier_semaphore()
    n_peers = tab[PEERS]

    @pl.loop(0, n_peers)
    def _(i):
        pl.semaphore_signal(
            barrier, 1, device_id=(tab[starts["peers"] + i], c),
            device_id_type=pl.DeviceIdType.MESH,
        )

    for k in range(1, 4):
        pl.semaphore_signal(
            barrier, 1, device_id=(r, lax.rem(c + k, 4)), device_id_type=pl.DeviceIdType.MESH
        )

    n_made = tab[MADE_COUNT]

    @pl.when(n_made > 0)
    def _():
        first = tab[MADE_FIRST] * 8
        line, shift = first // LINES, lax.rem(first, LINES)
        after = jnp.minimum(line + 1, DEVICES - 1)
        lane = lax.broadcasted_iota(jnp.int32, (1, LINES), 1)

        def aligned(ref):
            one = pltpu.roll(jnp.broadcast_to(ref[pl.ds(line, 1), :], (8, LINES)), LINES - shift, 1)
            two = pltpu.roll(jnp.broadcast_to(ref[pl.ds(after, 1), :], (8, LINES)), LINES - shift, 1)
            return jnp.where(lane < LINES - shift, one[:1], two[:1])

        row = turned(aligned(low_ref))
        weight = turned(aligned(weight_ref))
        column = r * LINES + lax.broadcasted_iota(jnp.int32, (LINES, LINES), 1)
        values = jnp.where(row == column, weight, 0.0) + jnp.where(row + 1 == column, 1.0 - weight, 0.0)
        w_made[pl.ds(0, LINES), :], w_made[pl.ds(LINES, LINES), :] = split(values)

    pl.semaphore_wait(barrier, n_peers + 3)

    def copy(j, at, q):
        slot, device, place = tab[at], tab[at + 1], tab[at + 2]
        return pltpu.make_async_remote_copy(
            src_ref=buf.at[q, slot],
            dst_ref=buf.at[q, place],
            send_sem=send_sem.at[j, q],
            recv_sem=take_sem.at[place - TAKEN, q],
            device_id=(device, c),
            device_id_type=pl.DeviceIdType.MESH,
        )

    def arrived(place, q):
        return pltpu.make_async_remote_copy(
            src_ref=buf.at[q, place],
            dst_ref=buf.at[q, place],
            send_sem=send_sem.at[0, q],
            recv_sem=take_sem.at[place - TAKEN, q],
            device_id=(r, lax.rem(c + 1, 4)),
            device_id_type=pl.DeviceIdType.MESH,
        )

    n_own, n_locals = tab[SENDS], tab[LOCALS]
    for q in range(CHUNKS):
        loads[q].wait()

        @pl.when(n_made > 0)
        def _():
            @pl.loop(0, CHUNK // STEP)
            def _(t):
                columns = pl.ds(pl.multiple_of(t * STEP, STEP), STEP)
                x = buf[q, pl.ds(OWN, 16), :, columns].reshape(LINES, STEP)
                made = weighted(w_made[...], x)
                buf[q, pl.ds(MADE, 16), :, columns] = made.reshape(16, 8, STEP)

        @pl.loop(0, n_own)
        def _(j):
            copy(j, starts["sends"] + 3 * j, q).start()

        @pl.loop(0, n_locals)
        def _(i):
            place = tab[starts["locals"] + 3 * i + 2]
            pltpu.make_async_copy(
                src.at[tab[starts["locals"] + 3 * i], :, chunk(q)],
                buf.at[q, place],
                take_sem.at[place - TAKEN, q],
            ).start()

    blended = r >= FIRST_BLENDED
    n_taken = tab[COUNT]
    a = lax.broadcasted_iota(jnp.int32, (256, 128), 0)
    b = lax.broadcasted_iota(jnp.int32, (256, 128), 1)
    pool[...] = jnp.where(a // 2 == b, 0.25, 0.0).astype(jnp.bfloat16)

    @pl.when(jnp.logical_or(r < FIRST_BLENDED, r >= FIRST_KEPT))
    def _():
        row = turned(low_ref[pl.ds(r, 1), :]) - tab[BASE]
        weight = turned(weight_ref[pl.ds(r, 1), :])
        row = jnp.concatenate([row, row], axis=1)
        weight = jnp.concatenate([weight, weight], axis=1)
        column = lax.broadcasted_iota(jnp.int32, (LINES, 2 * LINES), 1)
        values = jnp.where(row == column, weight, 0.0) + jnp.where(row + 1 == column, 1.0 - weight, 0.0)
        high, low = split(values[:, : 8 * RECEIVED])
        w_take[pl.ds(0, LINES), :] = high
        w_take[pl.ds(LINES, LINES), :] = low

    n_early, n_relays = tab[EARLY], tab[RELAYS]

    def forward(j, q):
        at = starts["relays"] + 3 * j
        arrived(tab[at], q).wait_recv()
        copy(n_sends + j, at, q).start()

    for q in range(CHUNKS + 1):
        if q < CHUNKS:
            @pl.loop(0, n_early)
            def _(j):
                forward(j, q)
        if q > 0:
            @pl.loop(n_early, n_relays)
            def _(j):
                forward(j, q - 1)

    def pool_columns(blocks):
        rows = blocks[0].shape[0]
        high, low = split(jnp.concatenate(blocks, axis=0))
        both = mm(high, pool[...]) + mm(low, pool[...])
        return [both[rows * i : rows * i + rows] for i in range(len(blocks))]

    def halve(tiles, count, rows):
        def one(i):
            return tiles[i, pl.ds(0, rows, 2), :] + tiles[i, pl.ds(1, rows, 2), :]

        return pool_columns(
            [jnp.concatenate([one(i), one(i + 1)], axis=1) for i in range(0, count, 2)]
        )

    for q in range(CHUNKS):
        for span in (SPANS, SPANS + 2):
            @pl.loop(tab[span], tab[span + 1])
            def _(i):
                arrived(TAKEN + i, q).wait_recv()

        @pl.when(jnp.logical_not(blended))
        def _():
            for t in range(0, CHUNK, STEP):
                x = buf[q, pl.ds(TAKEN, RECEIVED), :, pl.ds(t, STEP)].reshape(8 * RECEIVED, STEP)
                x = jnp.where(lax.broadcasted_iota(jnp.int32, x.shape, 0) < 8 * n_taken, x, 0.0)
                merc[:, pl.ds(q * CHUNK + t, STEP)] = weighted(w_take[...], x)

        @pl.when(blended)
        def _():
            @pl.when(r < FIRST_KEPT)
            def _():
                merc[:, chunk(q)] = buf[q, pl.ds(TAKEN, 16)].reshape(LINES, CHUNK)

            @pl.when(r >= FIRST_KEPT)
            def _():
                for t in range(0, CHUNK, STEP):
                    x = buf[q, pl.ds(TAKEN, 16), :, pl.ds(t, STEP)].reshape(LINES, STEP)
                    x = jnp.where(lax.broadcasted_iota(jnp.int32, x.shape, 0) < 8 * tab[SPANS + 1], x, 0.0)
                    own = buf[q, pl.ds(OWN, 16), :, pl.ds(t, STEP)].reshape(LINES, STEP)
                    merc[:, pl.ds(q * CHUNK + t, STEP)] = x + weighted(w_take[:, :LINES], own)

            for i in range(most_extra):
                @pl.when(i < tab[EXTRAS])
                def _():
                    rows = pl.ds(pl.multiple_of(tab[starts["extra"] + i] * 8, 8), 8)
                    merc[rows, chunk(q)] += buf[q, TAKEN + 16 + i]

        for i in range(CHUNK // 128):
            tiles0[i] = merc[:, pl.ds(q * CHUNK + 128 * i, 128)]
        for i, part in enumerate(halve(tiles0, CHUNK // 128, 64)):
            tiles1[i] = part
            out1[:, pl.ds(q * CHUNK // 2 + 128 * i, 128)] = part
        for i, part in enumerate(halve(tiles1, CHUNK // 256, 32)):
            tiles2[i] = part
            out2[:, pl.ds(q * CHUNK // 4 + 128 * i, 128)] = part
        for i, part in enumerate(halve(tiles2, CHUNK // 512, 16)):
            for k in range(4):
                l3_send[k, :, pl.ds(q * CHUNK // 8 + 128 * i, 128)] = part[4 * k : 4 * k + 4]

    ys = []
    for k in range(1, 4):
        other = lax.rem(c + k, 4)
        ys.append(
            pltpu.make_async_remote_copy(
                src_ref=l3_send.at[other],
                dst_ref=l3_take.at[c],
                send_sem=y_send_sem.at[k - 1],
                recv_sem=y_take_sem.at[k - 1],
                device_id=(r, other),
                device_id_type=pl.DeviceIdType.MESH,
            )
        )
    for y in ys:
        y.start()
    for y in ys:
        y.wait_recv()
    for k in range(4):
        out3[:, pl.ds(k * WIDTH // 8, WIDTH // 8)] = jnp.where(c == k, l3_send[k], l3_take[k])
    level3 = out3[...]
    sums = jnp.concatenate(
        [level3[0:1] + level3[1:2], level3[2:3] + level3[3:4], jnp.zeros((6, WIDTH // 2), jnp.float32)],
        axis=0,
    )
    for i, part in enumerate(pool_columns([sums[:, 256 * i : 256 * i + 256] for i in range(16)])):
        out4[:, pl.ds(128 * i, 128)] = part[:2]

    for y in ys:
        y.wait_send()
    for q in range(CHUNKS):
        @pl.loop(0, n_own)
        def _(j):
            copy(j, starts["sends"] + 3 * j, q).wait_send()

        @pl.loop(0, n_relays)
        def _(j):
            copy(n_sends + j, starts["relays"] + 3 * j, q).wait_send()


def store(*refs):
    *arrays, sems = refs
    copies = []
    for i in range(4):
        rows = pl.ds(32 * i, 32)
        copies.append(pltpu.make_async_copy(arrays[0].at[rows], arrays[5].at[rows], sems.at[i]))
    for i in range(1, 5):
        copies.append(pltpu.make_async_copy(arrays[i], arrays[5 + i], sems.at[3 + i]))
    for copy in copies:
        copy.start()
    for copy in copies:
        copy.wait()


def body(source, low_row, weight_low):
    words, starts, size, most_passed, n_sends, n_relays = make_tables()
    slots = PASSED + most_passed
    f32 = jnp.float32
    vmem = pl.BlockSpec(memory_space=pltpu.VMEM)
    results = pl.pallas_call(
        functools.partial(kernel, words, starts, n_sends, starts["peers"] - starts["extra"]),
        out_shape=(
            jax.ShapeDtypeStruct((128, 8192), f32),
            jax.ShapeDtypeStruct((64, 4096), f32),
            jax.ShapeDtypeStruct((32, 2048), f32),
            jax.ShapeDtypeStruct((4, 4096), f32),
            jax.ShapeDtypeStruct((2, 2048), f32),
        ),
        in_specs=[pl.BlockSpec(memory_space=pl.ANY), vmem, vmem],
        out_specs=(vmem,) * 5,
        scratch_shapes=[
            pltpu.VMEM((CHUNKS, slots, 8, CHUNK), f32),
            pltpu.SMEM((size,), jnp.int32),
            pltpu.VMEM((2 * LINES, LINES), jnp.bfloat16),
            pltpu.VMEM((2 * LINES, 8 * RECEIVED), jnp.bfloat16),
            pltpu.VMEM((256, 128), jnp.bfloat16),
            pltpu.VMEM((CHUNK // 128, 128, 128), f32),
            pltpu.VMEM((CHUNK // 256, 64, 128), f32),
            pltpu.VMEM((CHUNK // 512, 32, 128), f32),
            pltpu.VMEM((4, 4, WIDTH // 8), f32),
            pltpu.VMEM((4, 4, WIDTH // 8), f32),
            pltpu.SemaphoreType.DMA((CHUNKS,)),
            pltpu.SemaphoreType.DMA((n_sends + n_relays, CHUNKS)),
            pltpu.SemaphoreType.DMA((RECEIVED + most_passed, CHUNKS)),
            pltpu.SemaphoreType.DMA((3,)),
            pltpu.SemaphoreType.DMA((3,)),
        ],
        compiler_params=pltpu.CompilerParams(
            collective_id=0, has_side_effects=True, vmem_limit_bytes=48 * 2**20
        ),
    )(source.reshape(16, 8, WIDTH), low_row.reshape(64, 128), weight_low.reshape(64, 128))
    return pl.pallas_call(
        store,
        out_shape=tuple(jax.ShapeDtypeStruct(v.shape, v.dtype) for v in results),
        in_specs=[vmem] * 5,
        out_specs=(pl.BlockSpec(memory_space=pl.ANY),) * 5,
        scratch_shapes=[pltpu.SemaphoreType.DMA((8,))],
        compiler_params=pltpu.CompilerParams(vmem_limit_bytes=2**20),
    )(*results)


def solution(mesh):
    placed = (P("rows", "cols"), P(), P())
    return jax.shard_map(
        body,
        mesh=mesh,
        in_specs=placed,
        out_specs=(
            P("rows", "cols"),
            P("rows", "cols"),
            P("rows", "cols"),
            P(("rows", "cols"), None),
            P(("rows", "cols"), None),
        ),
        check_vma=False,
    )
```

```python
import functools
import math

import jax
import jax.numpy as jnp
import numpy as np
from jax import lax
from jax.experimental import pallas as pl
from jax.experimental.pallas import tpu as pltpu
from jax.sharding import PartitionSpec as P

TOTAL = 8192
WIDTH = 8192
LINES = 128
DEVICES = 64
FIRST_BLENDED = 36
FIRST_KEPT = 61
CHUNKS = 4
CHUNK = WIDTH // CHUNKS
STEP = 1024

ROUTES = (
    ((2, 0, 4), 1),
    ((3, 0, 5), 12),
    ((4, 11, 7), 2),
    ((5, 4, 8), 19),
    ((6, 5, 9), 11),
    ((7, 4, 11), 1),
    ((7, 23, 11), 7),
    ((9, 29, 13), 7),
    ((10, 30, 14), 7),
    ((11, 31, 15), 9),
    ((12, 28, 16), 5),
    ((13, 29, 17), 7),
    ((14, 30, 17), 4),
    ((15, 31, 18), 5),
    ((17, 19, 20), 2),
    ((18, 16, 21), 3),
    ((19, 16, 22), 5),
    ((20, 27, 23), 4),
    ((21, 22, 23), 7),
    ((21, 20, 24), 9),
    ((21, 28, 24), 8),
    ((22, 20, 24), 7),
    ((22, 21, 25), 4),
    ((23, 24, 25), 6),
    ((24, 22, 26), 9),
    ((25, 26, 27), 1),
    ((26, 1, 28), 1),
    ((27, 24, 28), 9),
    ((28, 1, 29), 2),
)

RECEIVED = 20
OWN, MADE, TAKEN = 0, 16, 32
PASSED = TAKEN + RECEIVED


def row_range():
    top = 68.0 * math.pi / 180.0
    edge = math.log(math.tan(math.pi / 4 + top / 2))
    rows = np.arange(TOTAL)
    lat = 2.0 * np.arctan(np.exp(edge * (1.0 - (2 * rows + 1) / (2.0 * TOTAL)))) - math.pi / 2
    place = (top - lat) / top * TOTAL - 0.5
    first = np.clip(np.floor(place - 0.05), 0, TOTAL - 2).astype(int)
    last = np.clip(np.floor(place + 0.05), 0, TOTAL - 2).astype(int)
    return np.clip(first - 2, 0, TOTAL - 2), np.clip(last + 2, 0, TOTAL - 2) + 1


@functools.cache
def make_plan():
    low, high = row_range()
    flows = []
    head = [dict(sends=[], relays=[], locals=[], peers=set()) for _ in range(DEVICES)]
    made_first = {}
    for d in range(FIRST_BLENDED, DEVICES):
        for q in range(16 * d, 16 * d + 16):
            for s in range(low[8 * q] // LINES, min(high[8 * q + 7] // LINES, d - 1) + 1):
                made_first[s] = min(made_first.get(s, q), q)
    for r, h in enumerate(head):
        h["made_first"] = made_first.get(r, 0)
        h["made"] = 0
        h["extra"] = []
        h["used"] = [False] * RECEIVED
    for d in range(DEVICES):
        h = head[d]
        if d < FIRST_BLENDED:
            first, last = low[LINES * d] // 8, high[LINES * d + LINES - 1] // 8
            h["base"] = 8 * first
            h["count"] = last - first + 1
            for g in range(first, last + 1):
                flows.append((g // 16, d, OWN + g % 16, TAKEN + g - first))
        else:
            h["base"] = LINES * d
            for q in range(16 * d, 16 * d + 16):
                for n, s in enumerate(range(low[8 * q] // LINES, high[8 * q + 7] // LINES + 1)):
                    if s == d:
                        continue
                    place = q - made_first[s]
                    head[s]["made"] = max(head[s]["made"], place + 1)
                    if n == 0:
                        slot = q - 16 * d
                    else:
                        slot = 16 + len(h["extra"])
                        h["extra"].append(q - 16 * d)
                    flows.append((s, d, MADE + place, TAKEN + slot))
            h["count"] = 16 + len(h["extra"])
    between = {}
    for s, d, _, _ in flows:
        between[s // 2, d // 2] = between.get((s // 2, d // 2), 0) + 1
    ways = {}
    for way, blocks in ROUTES:
        ways.setdefault((way[0], way[-1]), []).append([blocks, way])
    routes = {}
    for pair, total in between.items():
        counts = ways.get(pair, [])
        rest = total - sum(n for n, _ in counts)
        assert rest >= 0
        marks = [((i + 0.5) / n, way) for n, way in counts + [[rest, pair]] for i in range(n)]
        routes[pair] = [way for _, way in sorted(marks)]
    loads, sides = [0] * DEVICES, {}
    for way, blocks in sorted(ROUTES, key=lambda v: -v[1]):
        for chip in way[1:-1]:
            sides[way, chip] = int(loads[2 * chip + 1] < loads[2 * chip])
            loads[2 * chip + sides[way, chip]] += blocks
    passed = [0] * DEVICES
    for s, d, slot, goal in flows:
        head[d]["used"][goal - TAKEN] = True
        if s == d:
            head[s]["locals"].append((slot, goal))
            routes[s // 2, d // 2].pop()
            continue
        way = routes[s // 2, d // 2].pop()
        stops = []
        for chip in way[1:-1]:
            stop = 2 * chip + sides[way, chip]
            stops.append((stop, PASSED + passed[stop]))
            passed[stop] += 1
        stops.append((d, goal))
        at = s
        for leg, (stop, place) in enumerate(stops):
            if leg == 0:
                head[s]["sends"].append((-len(stops), slot, stop, place))
            else:
                head[at]["relays"].append((leg, -len(stops), slot, stop, place))
            head[at]["peers"].add(stop)
            head[stop]["peers"].add(at)
            at, slot = stop, place
    assert not any(routes.values())
    for h in head:
        inner = [i for i in range(16) if h["used"][i]]
        outer = [i for i in range(16, RECEIVED) if h["used"][i]]
        h["spans"] = []
        for some in (inner, outer):
            h["spans"] += [some[0], some[-1] + 1] if some else [0, 0]
            assert not some or len(some) == some[-1] + 1 - some[0]
        turns, seen = [], {}
        for stops, *move in sorted(h["sends"], key=lambda v: v[0]):
            key = stops, move[1]
            seen[key] = seen.get(key, 0) + 1
            turns.append((stops == -1, key, seen[key], move))
        h["sends"] = [
            move for _, _, _, move in sorted(turns, key=lambda v: (v[0], (v[2] - 0.5) / seen[v[1]], v[1]))
        ]
        relays = sorted(h["relays"])
        h["early"] = sum(v[0] == 1 for v in relays)
        h["relays"] = [v[2:] for v in relays]
        h["peers"] = sorted(h["peers"])
    return head, max(passed)


(SENDS, EARLY, RELAYS, LOCALS, COUNT, MADE_COUNT, MADE_FIRST, BASE, EXTRAS, PEERS) = range(10)
SPANS, LISTS = 10, 14


def make_tables():
    head, most_passed = make_plan()
    width = lambda name: max(len(h[name]) for h in head)
    starts, at = {}, LISTS
    for name in ("extra", "peers", "locals", "sends", "relays"):
        starts[name] = at
        at += width(name) * (3 if name in ("locals", "sends", "relays") else 1)
    words = []
    for h in head:
        w = [None] * at
        w[SENDS], w[EARLY], w[RELAYS] = len(h["sends"]), h["early"], len(h["relays"])
        w[LOCALS], w[COUNT] = len(h["locals"]), int(h["count"])
        w[MADE_COUNT], w[MADE_FIRST] = int(h["made"]), int(h["made_first"])
        w[BASE], w[EXTRAS], w[PEERS] = int(h["base"]), len(h["extra"]), len(h["peers"])
        w[SPANS : SPANS + 4] = [int(v) for v in h["spans"]]
        for name in ("extra", "peers"):
            for i, v in enumerate(h[name]):
                w[starts[name] + i] = int(v)
        for i, (slot, place) in enumerate(h["locals"]):
            w[starts["locals"] + 3 * i : starts["locals"] + 3 * i + 3] = [int(slot), 0, int(place)]
        for name in ("sends", "relays"):
            for i, v in enumerate(h[name]):
                w[starts[name] + 3 * i : starts[name] + 3 * i + 3] = [int(x) for x in v]
        words.append(w)
    return words, starts, at, most_passed, width("sends"), width("relays")


def split(x):
    high = x.astype(jnp.bfloat16)
    return high, (x - high.astype(jnp.float32)).astype(jnp.bfloat16)


def mm(a, b):
    return jnp.dot(a, b, preferred_element_type=jnp.float32)


def weighted(weights, x):
    high, low = split(x)
    both = mm(weights, high)
    return both[:LINES] + both[LINES:] + mm(weights[:LINES], low)


def turned(row):
    return jnp.transpose(jnp.broadcast_to(row, (LINES, LINES)))


def kernel(
    words, starts, n_sends, most_extra,
    src, low_ref, weight_ref,
    merc, out1, out2, out3, out4,
    buf, tab, w_made, w_take, pool, tiles0, tiles1, tiles2, l3_send, l3_take,
    load_sem, send_sem, take_sem, y_send_sem, y_take_sem,
):
    r = lax.axis_index("rows")
    c = lax.axis_index("cols")

    def fill(low_half, count):
        if count == 1:
            for i, v in enumerate(words[low_half]):
                if v is not None:
                    tab[i] = v
            return
        half = count // 2
        lax.cond(
            r < low_half + half,
            lambda: fill(low_half, half),
            lambda: fill(low_half + half, half),
        )

    fill(0, DEVICES)

    def chunk(q):
        return pl.ds(q * CHUNK, CHUNK)

    loads = [
        pltpu.make_async_copy(
            src.at[:, :, chunk(q)], buf.at[q, pl.ds(OWN, 16)], load_sem.at[q]
        )
        for q in range(CHUNKS)
    ]
    for load in loads:
        load.start()

    barrier = pltpu.get_barrier_semaphore()
    n_peers = tab[PEERS]

    @pl.loop(0, n_peers)
    def _(i):
        pl.semaphore_signal(
            barrier, 1, device_id=(tab[starts["peers"] + i], c),
            device_id_type=pl.DeviceIdType.MESH,
        )

    for k in range(1, 4):
        pl.semaphore_signal(
            barrier, 1, device_id=(r, lax.rem(c + k, 4)), device_id_type=pl.DeviceIdType.MESH
        )

    n_made = tab[MADE_COUNT]

    @pl.when(n_made > 0)
    def _():
        first = tab[MADE_FIRST] * 8
        line, shift = first // LINES, lax.rem(first, LINES)
        after = jnp.minimum(line + 1, DEVICES - 1)
        lane = lax.broadcasted_iota(jnp.int32, (1, LINES), 1)

        def aligned(ref):
            one = pltpu.roll(jnp.broadcast_to(ref[pl.ds(line, 1), :], (8, LINES)), LINES - shift, 1)
            two = pltpu.roll(jnp.broadcast_to(ref[pl.ds(after, 1), :], (8, LINES)), LINES - shift, 1)
            return jnp.where(lane < LINES - shift, one[:1], two[:1])

        row = turned(aligned(low_ref))
        weight = turned(aligned(weight_ref))
        column = r * LINES + lax.broadcasted_iota(jnp.int32, (LINES, LINES), 1)
        values = jnp.where(row == column, weight, 0.0) + jnp.where(row + 1 == column, 1.0 - weight, 0.0)
        w_made[pl.ds(0, LINES), :], w_made[pl.ds(LINES, LINES), :] = split(values)

    pl.semaphore_wait(barrier, n_peers + 3)

    def copy(j, at, q):
        slot, device, place = tab[at], tab[at + 1], tab[at + 2]
        return pltpu.make_async_remote_copy(
            src_ref=buf.at[q, slot],
            dst_ref=buf.at[q, place],
            send_sem=send_sem.at[j, q],
            recv_sem=take_sem.at[place - TAKEN, q],
            device_id=(device, c),
            device_id_type=pl.DeviceIdType.MESH,
        )

    def arrived(place, q):
        return pltpu.make_async_remote_copy(
            src_ref=buf.at[q, place],
            dst_ref=buf.at[q, place],
            send_sem=send_sem.at[0, q],
            recv_sem=take_sem.at[place - TAKEN, q],
            device_id=(r, lax.rem(c + 1, 4)),
            device_id_type=pl.DeviceIdType.MESH,
        )

    n_own, n_locals = tab[SENDS], tab[LOCALS]
    for q in range(CHUNKS):
        loads[q].wait()

        @pl.when(n_made > 0)
        def _():
            @pl.loop(0, CHUNK // STEP)
            def _(t):
                columns = pl.ds(pl.multiple_of(t * STEP, STEP), STEP)
                x = buf[q, pl.ds(OWN, 16), :, columns].reshape(LINES, STEP)
                made = weighted(w_made[...], x)
                buf[q, pl.ds(MADE, 16), :, columns] = made.reshape(16, 8, STEP)

        @pl.loop(0, n_own)
        def _(j):
            copy(j, starts["sends"] + 3 * j, q).start()

        @pl.loop(0, n_locals)
        def _(i):
            place = tab[starts["locals"] + 3 * i + 2]
            pltpu.make_async_copy(
                src.at[tab[starts["locals"] + 3 * i], :, chunk(q)],
                buf.at[q, place],
                take_sem.at[place - TAKEN, q],
            ).start()

    blended = r >= FIRST_BLENDED
    n_taken = tab[COUNT]
    a = lax.broadcasted_iota(jnp.int32, (256, 128), 0)
    b = lax.broadcasted_iota(jnp.int32, (256, 128), 1)
    pool[...] = jnp.where(a // 2 == b, 0.25, 0.0).astype(jnp.bfloat16)

    @pl.when(jnp.logical_or(r < FIRST_BLENDED, r >= FIRST_KEPT))
    def _():
        row = turned(low_ref[pl.ds(r, 1), :]) - tab[BASE]
        weight = turned(weight_ref[pl.ds(r, 1), :])
        row = jnp.concatenate([row, row], axis=1)
        weight = jnp.concatenate([weight, weight], axis=1)
        column = lax.broadcasted_iota(jnp.int32, (LINES, 2 * LINES), 1)
        values = jnp.where(row == column, weight, 0.0) + jnp.where(row + 1 == column, 1.0 - weight, 0.0)
        high, low = split(values[:, : 8 * RECEIVED])
        w_take[pl.ds(0, LINES), :] = high
        w_take[pl.ds(LINES, LINES), :] = low

    n_early, n_relays = tab[EARLY], tab[RELAYS]

    def forward(j, q):
        at = starts["relays"] + 3 * j
        arrived(tab[at], q).wait_recv()
        copy(n_sends + j, at, q).start()

    for q in range(CHUNKS + 1):
        if q < CHUNKS:
            @pl.loop(0, n_early)
            def _(j):
                forward(j, q)
        if q > 0:
            @pl.loop(n_early, n_relays)
            def _(j):
                forward(j, q - 1)

    def pool_columns(blocks):
        rows = blocks[0].shape[0]
        high, low = split(jnp.concatenate(blocks, axis=0))
        both = mm(high, pool[...]) + mm(low, pool[...])
        return [both[rows * i : rows * i + rows] for i in range(len(blocks))]

    def halve(tiles, count, rows):
        def one(i):
            return tiles[i, pl.ds(0, rows, 2), :] + tiles[i, pl.ds(1, rows, 2), :]

        return pool_columns(
            [jnp.concatenate([one(i), one(i + 1)], axis=1) for i in range(0, count, 2)]
        )

    for q in range(CHUNKS):
        for span in (SPANS, SPANS + 2):
            @pl.loop(tab[span], tab[span + 1])
            def _(i):
                arrived(TAKEN + i, q).wait_recv()

        @pl.when(jnp.logical_not(blended))
        def _():
            for t in range(0, CHUNK, STEP):
                x = buf[q, pl.ds(TAKEN, RECEIVED), :, pl.ds(t, STEP)].reshape(8 * RECEIVED, STEP)
                x = jnp.where(lax.broadcasted_iota(jnp.int32, x.shape, 0) < 8 * n_taken, x, 0.0)
                merc[:, pl.ds(q * CHUNK + t, STEP)] = weighted(w_take[...], x)

        @pl.when(blended)
        def _():
            @pl.when(r < FIRST_KEPT)
            def _():
                merc[:, chunk(q)] = buf[q, pl.ds(TAKEN, 16)].reshape(LINES, CHUNK)

            @pl.when(r >= FIRST_KEPT)
            def _():
                for t in range(0, CHUNK, STEP):
                    x = buf[q, pl.ds(TAKEN, 16), :, pl.ds(t, STEP)].reshape(LINES, STEP)
                    x = jnp.where(lax.broadcasted_iota(jnp.int32, x.shape, 0) < 8 * tab[SPANS + 1], x, 0.0)
                    own = buf[q, pl.ds(OWN, 16), :, pl.ds(t, STEP)].reshape(LINES, STEP)
                    merc[:, pl.ds(q * CHUNK + t, STEP)] = x + weighted(w_take[:, :LINES], own)

            for i in range(most_extra):
                @pl.when(i < tab[EXTRAS])
                def _():
                    rows = pl.ds(pl.multiple_of(tab[starts["extra"] + i] * 8, 8), 8)
                    merc[rows, chunk(q)] += buf[q, TAKEN + 16 + i]

        for i in range(CHUNK // 128):
            tiles0[i] = merc[:, pl.ds(q * CHUNK + 128 * i, 128)]
        for i, part in enumerate(halve(tiles0, CHUNK // 128, 64)):
            tiles1[i] = part
            out1[:, pl.ds(q * CHUNK // 2 + 128 * i, 128)] = part
        for i, part in enumerate(halve(tiles1, CHUNK // 256, 32)):
            tiles2[i] = part
            out2[:, pl.ds(q * CHUNK // 4 + 128 * i, 128)] = part
        for i, part in enumerate(halve(tiles2, CHUNK // 512, 16)):
            for k in range(4):
                l3_send[k, :, pl.ds(q * CHUNK // 8 + 128 * i, 128)] = part[4 * k : 4 * k + 4]

    ys = []
    for k in range(1, 4):
        other = lax.rem(c + k, 4)
        ys.append(
            pltpu.make_async_remote_copy(
                src_ref=l3_send.at[other],
                dst_ref=l3_take.at[c],
                send_sem=y_send_sem.at[k - 1],
                recv_sem=y_take_sem.at[k - 1],
                device_id=(r, other),
                device_id_type=pl.DeviceIdType.MESH,
            )
        )
    for y in ys:
        y.start()
    for y in ys:
        y.wait_recv()
    for k in range(4):
        out3[:, pl.ds(k * WIDTH // 8, WIDTH // 8)] = jnp.where(c == k, l3_send[k], l3_take[k])
    level3 = out3[...]
    sums = jnp.concatenate(
        [level3[0:1] + level3[1:2], level3[2:3] + level3[3:4], jnp.zeros((6, WIDTH // 2), jnp.float32)],
        axis=0,
    )
    for i, part in enumerate(pool_columns([sums[:, 256 * i : 256 * i + 256] for i in range(16)])):
        out4[:, pl.ds(128 * i, 128)] = part[:2]

    for y in ys:
        y.wait_send()
    for q in range(CHUNKS):
        @pl.loop(0, n_own)
        def _(j):
            copy(j, starts["sends"] + 3 * j, q).wait_send()

        @pl.loop(0, n_relays)
        def _(j):
            copy(n_sends + j, starts["relays"] + 3 * j, q).wait_send()


def store(*refs):
    *arrays, sems = refs
    copies = []
    for i in range(4):
        rows = pl.ds(32 * i, 32)
        copies.append(pltpu.make_async_copy(arrays[0].at[rows], arrays[5].at[rows], sems.at[i]))
    for i in range(1, 5):
        copies.append(pltpu.make_async_copy(arrays[i], arrays[5 + i], sems.at[3 + i]))
    for copy in copies:
        copy.start()
    for copy in copies:
        copy.wait()


def body(source, low_row, weight_low):
    words, starts, size, most_passed, n_sends, n_relays = make_tables()
    slots = PASSED + most_passed
    f32 = jnp.float32
    vmem = pl.BlockSpec(memory_space=pltpu.VMEM)
    results = pl.pallas_call(
        functools.partial(kernel, words, starts, n_sends, starts["peers"] - starts["extra"]),
        out_shape=(
            jax.ShapeDtypeStruct((128, 8192), f32),
            jax.ShapeDtypeStruct((64, 4096), f32),
            jax.ShapeDtypeStruct((32, 2048), f32),
            jax.ShapeDtypeStruct((4, 4096), f32),
            jax.ShapeDtypeStruct((2, 2048), f32),
        ),
        in_specs=[pl.BlockSpec(memory_space=pl.ANY), vmem, vmem],
        out_specs=(vmem,) * 5,
        scratch_shapes=[
            pltpu.VMEM((CHUNKS, slots, 8, CHUNK), f32),
            pltpu.SMEM((size,), jnp.int32),
            pltpu.VMEM((2 * LINES, LINES), jnp.bfloat16),
            pltpu.VMEM((2 * LINES, 8 * RECEIVED), jnp.bfloat16),
            pltpu.VMEM((256, 128), jnp.bfloat16),
            pltpu.VMEM((CHUNK // 128, 128, 128), f32),
            pltpu.VMEM((CHUNK // 256, 64, 128), f32),
            pltpu.VMEM((CHUNK // 512, 32, 128), f32),
            pltpu.VMEM((4, 4, WIDTH // 8), f32),
            pltpu.VMEM((4, 4, WIDTH // 8), f32),
            pltpu.SemaphoreType.DMA((CHUNKS,)),
            pltpu.SemaphoreType.DMA((n_sends + n_relays, CHUNKS)),
            pltpu.SemaphoreType.DMA((RECEIVED + most_passed, CHUNKS)),
            pltpu.SemaphoreType.DMA((3,)),
            pltpu.SemaphoreType.DMA((3,)),
        ],
        compiler_params=pltpu.CompilerParams(
            collective_id=0, has_side_effects=True, vmem_limit_bytes=48 * 2**20
        ),
    )(source.reshape(16, 8, WIDTH), low_row.reshape(64, 128), weight_low.reshape(64, 128))
    return pl.pallas_call(
        store,
        out_shape=tuple(jax.ShapeDtypeStruct(v.shape, v.dtype) for v in results),
        in_specs=[vmem] * 5,
        out_specs=(pl.BlockSpec(memory_space=pl.ANY),) * 5,
        scratch_shapes=[pltpu.SemaphoreType.DMA((8,))],
        compiler_params=pltpu.CompilerParams(vmem_limit_bytes=2**20),
    )(*results)


def solution(mesh):
    placed = (P("rows", "cols"), P(), P())
    return jax.shard_map(
        body,
        mesh=mesh,
        in_specs=placed,
        out_specs=(
            P("rows", "cols"),
            P("rows", "cols"),
            P("rows", "cols"),
            P(("rows", "cols"), None),
            P(("rows", "cols"), None),
        ),
        check_vma=False,
    )
```

```python
import functools
import math

import jax
import jax.numpy as jnp
import numpy as np
from jax import lax
from jax.experimental import pallas as pl
from jax.experimental.pallas import tpu as pltpu
from jax.sharding import PartitionSpec as P

TOTAL = 8192
WIDTH = 8192
LINES = 128
DEVICES = 64
FIRST_BLENDED = 36
FIRST_KEPT = 61
CHUNKS = 4
CHUNK = WIDTH // CHUNKS
STEP = 1024

ROUTES = (
    ((2, 0, 4), 1),
    ((3, 0, 5), 12),
    ((4, 11, 7), 2),
    ((5, 4, 8), 19),
    ((6, 5, 9), 11),
    ((7, 4, 11), 1),
    ((7, 23, 11), 7),
    ((9, 29, 13), 7),
    ((10, 30, 14), 7),
    ((11, 31, 15), 9),
    ((12, 28, 16), 5),
    ((13, 29, 17), 7),
    ((14, 30, 17), 4),
    ((15, 31, 18), 5),
    ((17, 19, 20), 2),
    ((18, 16, 21), 3),
    ((19, 16, 22), 5),
    ((20, 27, 23), 4),
    ((21, 22, 23), 7),
    ((21, 20, 24), 9),
    ((21, 28, 24), 8),
    ((22, 20, 24), 7),
    ((22, 21, 25), 4),
    ((23, 24, 25), 6),
    ((24, 22, 26), 9),
    ((25, 26, 27), 1),
    ((26, 1, 28), 1),
    ((27, 24, 28), 9),
    ((28, 1, 29), 2),
)

RECEIVED = 20
OWN, MADE, TAKEN = 0, 16, 32
PASSED = TAKEN + RECEIVED


def row_range():
    top = 68.0 * math.pi / 180.0
    edge = math.log(math.tan(math.pi / 4 + top / 2))
    rows = np.arange(TOTAL)
    lat = 2.0 * np.arctan(np.exp(edge * (1.0 - (2 * rows + 1) / (2.0 * TOTAL)))) - math.pi / 2
    place = (top - lat) / top * TOTAL - 0.5
    first = np.clip(np.floor(place - 0.05), 0, TOTAL - 2).astype(int)
    last = np.clip(np.floor(place + 0.05), 0, TOTAL - 2).astype(int)
    return np.clip(first - 2, 0, TOTAL - 2), np.clip(last + 2, 0, TOTAL - 2) + 1


@functools.cache
def make_plan():
    low, high = row_range()
    flows = []
    head = [dict(sends=[], relays=[], locals=[], peers=set()) for _ in range(DEVICES)]
    made_first = {}
    for d in range(FIRST_BLENDED, DEVICES):
        for q in range(16 * d, 16 * d + 16):
            for s in range(low[8 * q] // LINES, min(high[8 * q + 7] // LINES, d - 1) + 1):
                made_first[s] = min(made_first.get(s, q), q)
    for r, h in enumerate(head):
        h["made_first"] = made_first.get(r, 0)
        h["made"] = 0
        h["extra"] = []
        h["used"] = [False] * RECEIVED
    for d in range(DEVICES):
        h = head[d]
        if d < FIRST_BLENDED:
            first, last = low[LINES * d] // 8, high[LINES * d + LINES - 1] // 8
            h["base"] = 8 * first
            h["count"] = last - first + 1
            for g in range(first, last + 1):
                flows.append((g // 16, d, OWN + g % 16, TAKEN + g - first))
        else:
            h["base"] = LINES * d
            for q in range(16 * d, 16 * d + 16):
                for n, s in enumerate(range(low[8 * q] // LINES, high[8 * q + 7] // LINES + 1)):
                    if s == d:
                        continue
                    place = q - made_first[s]
                    head[s]["made"] = max(head[s]["made"], place + 1)
                    if n == 0:
                        slot = q - 16 * d
                    else:
                        slot = 16 + len(h["extra"])
                        h["extra"].append(q - 16 * d)
                    flows.append((s, d, MADE + place, TAKEN + slot))
            h["count"] = 16 + len(h["extra"])
    between = {}
    for s, d, _, _ in flows:
        between[s // 2, d // 2] = between.get((s // 2, d // 2), 0) + 1
    ways = {}
    for way, blocks in ROUTES:
        ways.setdefault((way[0], way[-1]), []).append([blocks, way])
    routes = {}
    for pair, total in between.items():
        counts = ways.get(pair, [])
        rest = total - sum(n for n, _ in counts)
        assert rest >= 0
        marks = [((i + 0.5) / n, way) for n, way in counts + [[rest, pair]] for i in range(n)]
        routes[pair] = [way for _, way in sorted(marks)]
    loads, sides = [0] * DEVICES, {}
    for way, blocks in sorted(ROUTES, key=lambda v: -v[1]):
        for chip in way[1:-1]:
            sides[way, chip] = int(loads[2 * chip + 1] < loads[2 * chip])
            loads[2 * chip + sides[way, chip]] += blocks
    passed = [0] * DEVICES
    for s, d, slot, goal in flows:
        head[d]["used"][goal - TAKEN] = True
        if s == d:
            head[s]["locals"].append((slot, goal))
            routes[s // 2, d // 2].pop()
            continue
        way = routes[s // 2, d // 2].pop()
        stops = []
        for chip in way[1:-1]:
            stop = 2 * chip + sides[way, chip]
            stops.append((stop, PASSED + passed[stop]))
            passed[stop] += 1
        stops.append((d, goal))
        at = s
        for leg, (stop, place) in enumerate(stops):
            if leg == 0:
                head[s]["sends"].append((-len(stops), slot, stop, place))
            else:
                head[at]["relays"].append((leg, -len(stops), slot, stop, place))
            head[at]["peers"].add(stop)
            head[stop]["peers"].add(at)
            at, slot = stop, place
    assert not any(routes.values())
    for h in head:
        inner = [i for i in range(16) if h["used"][i]]
        outer = [i for i in range(16, RECEIVED) if h["used"][i]]
        h["spans"] = []
        for some in (inner, outer):
            h["spans"] += [some[0], some[-1] + 1] if some else [0, 0]
            assert not some or len(some) == some[-1] + 1 - some[0]
        turns, seen = [], {}
        for stops, *move in sorted(h["sends"], key=lambda v: v[0]):
            key = stops, move[1]
            seen[key] = seen.get(key, 0) + 1
            turns.append((stops == -1, key, seen[key], move))
        h["sends"] = [
            move for _, _, _, move in sorted(turns, key=lambda v: (v[0], (v[2] - 0.5) / seen[v[1]], v[1]))
        ]
        relays = sorted(h["relays"])
        h["early"] = sum(v[0] == 1 for v in relays)
        h["relays"] = [v[2:] for v in relays]
        h["peers"] = sorted(h["peers"])
    return head, max(passed)


(SENDS, EARLY, RELAYS, LOCALS, COUNT, MADE_COUNT, MADE_FIRST, BASE, EXTRAS, PEERS) = range(10)
SPANS, LISTS = 10, 14


def make_tables():
    head, most_passed = make_plan()
    width = lambda name: max(len(h[name]) for h in head)
    starts, at = {}, LISTS
    for name in ("extra", "peers", "locals", "sends", "relays"):
        starts[name] = at
        at += width(name) * (3 if name in ("locals", "sends", "relays") else 1)
    words = []
    for h in head:
        w = [None] * at
        w[SENDS], w[EARLY], w[RELAYS] = len(h["sends"]), h["early"], len(h["relays"])
        w[LOCALS], w[COUNT] = len(h["locals"]), int(h["count"])
        w[MADE_COUNT], w[MADE_FIRST] = int(h["made"]), int(h["made_first"])
        w[BASE], w[EXTRAS], w[PEERS] = int(h["base"]), len(h["extra"]), len(h["peers"])
        w[SPANS : SPANS + 4] = [int(v) for v in h["spans"]]
        for name in ("extra", "peers"):
            for i, v in enumerate(h[name]):
                w[starts[name] + i] = int(v)
        for i, (slot, place) in enumerate(h["locals"]):
            w[starts["locals"] + 3 * i : starts["locals"] + 3 * i + 3] = [int(slot), 0, int(place)]
        for name in ("sends", "relays"):
            for i, v in enumerate(h[name]):
                w[starts[name] + 3 * i : starts[name] + 3 * i + 3] = [int(x) for x in v]
        words.append(w)
    return words, starts, at, most_passed, width("sends"), width("relays")


def split(x):
    high = x.astype(jnp.bfloat16)
    return high, (x - high.astype(jnp.float32)).astype(jnp.bfloat16)


def mm(a, b):
    return jnp.dot(a, b, preferred_element_type=jnp.float32)


def weighted(weights, x):
    high, low = split(x)
    both = mm(weights, high)
    return both[:LINES] + both[LINES:] + mm(weights[:LINES], low)


def turned(row):
    return jnp.transpose(jnp.broadcast_to(row, (LINES, LINES)))


def kernel(
    words, starts, n_sends, most_extra,
    src, low_ref, weight_ref,
    merc, out1, out2, out3, out4,
    buf, tab, w_made, w_take, pool, tiles0, tiles1, tiles2, l3_send, l3_take,
    load_sem, send_sem, take_sem, y_send_sem, y_take_sem,
):
    r = lax.axis_index("rows")
    c = lax.axis_index("cols")

    def fill(low_half, count):
        if count == 1:
            for i, v in enumerate(words[low_half]):
                if v is not None:
                    tab[i] = v
            return
        half = count // 2
        lax.cond(
            r < low_half + half,
            lambda: fill(low_half, half),
            lambda: fill(low_half + half, half),
        )

    fill(0, DEVICES)

    def chunk(q):
        return pl.ds(q * CHUNK, CHUNK)

    loads = [
        pltpu.make_async_copy(
            src.at[:, :, chunk(q)], buf.at[q, pl.ds(OWN, 16)], load_sem.at[q]
        )
        for q in range(CHUNKS)
    ]
    for load in loads:
        load.start()

    barrier = pltpu.get_barrier_semaphore()
    n_peers = tab[PEERS]

    @pl.loop(0, n_peers)
    def _(i):
        pl.semaphore_signal(
            barrier, 1, device_id=(tab[starts["peers"] + i], c),
            device_id_type=pl.DeviceIdType.MESH,
        )

    for k in range(1, 4):
        pl.semaphore_signal(
            barrier, 1, device_id=(r, lax.rem(c + k, 4)), device_id_type=pl.DeviceIdType.MESH
        )

    n_made = tab[MADE_COUNT]

    @pl.when(n_made > 0)
    def _():
        first = tab[MADE_FIRST] * 8
        line, shift = first // LINES, lax.rem(first, LINES)
        after = jnp.minimum(line + 1, DEVICES - 1)
        lane = lax.broadcasted_iota(jnp.int32, (1, LINES), 1)

        def aligned(ref):
            one = pltpu.roll(jnp.broadcast_to(ref[pl.ds(line, 1), :], (8, LINES)), LINES - shift, 1)
            two = pltpu.roll(jnp.broadcast_to(ref[pl.ds(after, 1), :], (8, LINES)), LINES - shift, 1)
            return jnp.where(lane < LINES - shift, one[:1], two[:1])

        row = turned(aligned(low_ref))
        weight = turned(aligned(weight_ref))
        column = r * LINES + lax.broadcasted_iota(jnp.int32, (LINES, LINES), 1)
        values = jnp.where(row == column, weight, 0.0) + jnp.where(row + 1 == column, 1.0 - weight, 0.0)
        w_made[pl.ds(0, LINES), :], w_made[pl.ds(LINES, LINES), :] = split(values)

    def copy(j, at, q):
        slot, device, place = tab[at], tab[at + 1], tab[at + 2]
        return pltpu.make_async_remote_copy(
            src_ref=buf.at[q, slot],
            dst_ref=buf.at[q, place],
            send_sem=send_sem.at[j, q],
            recv_sem=take_sem.at[place - TAKEN, q],
            device_id=(device, c),
            device_id_type=pl.DeviceIdType.MESH,
        )

    def arrived(place, q):
        return pltpu.make_async_remote_copy(
            src_ref=buf.at[q, place],
            dst_ref=buf.at[q, place],
            send_sem=send_sem.at[0, q],
            recv_sem=take_sem.at[place - TAKEN, q],
            device_id=(r, lax.rem(c + 1, 4)),
            device_id_type=pl.DeviceIdType.MESH,
        )

    n_own, n_locals = tab[SENDS], tab[LOCALS]
    for q in range(CHUNKS):
        loads[q].wait()

        @pl.when(n_made > 0)
        def _():
            @pl.loop(0, CHUNK // STEP)
            def _(t):
                columns = pl.ds(pl.multiple_of(t * STEP, STEP), STEP)
                x = buf[q, pl.ds(OWN, 16), :, columns].reshape(LINES, STEP)
                made = weighted(w_made[...], x)
                buf[q, pl.ds(MADE, 16), :, columns] = made.reshape(16, 8, STEP)

        if q == 0:
            pl.semaphore_wait(barrier, n_peers + 3)

        @pl.loop(0, n_own)
        def _(j):
            copy(j, starts["sends"] + 3 * j, q).start()

        @pl.loop(0, n_locals)
        def _(i):
            place = tab[starts["locals"] + 3 * i + 2]
            pltpu.make_async_copy(
                src.at[tab[starts["locals"] + 3 * i], :, chunk(q)],
                buf.at[q, place],
                take_sem.at[place - TAKEN, q],
            ).start()

    blended = r >= FIRST_BLENDED
    n_taken = tab[COUNT]
    a = lax.broadcasted_iota(jnp.int32, (256, 128), 0)
    b = lax.broadcasted_iota(jnp.int32, (256, 128), 1)
    pool[...] = jnp.where(a // 2 == b, 0.25, 0.0).astype(jnp.bfloat16)

    @pl.when(jnp.logical_or(r < FIRST_BLENDED, r >= FIRST_KEPT))
    def _():
        row = turned(low_ref[pl.ds(r, 1), :]) - tab[BASE]
        weight = turned(weight_ref[pl.ds(r, 1), :])
        row = jnp.concatenate([row, row], axis=1)
        weight = jnp.concatenate([weight, weight], axis=1)
        column = lax.broadcasted_iota(jnp.int32, (LINES, 2 * LINES), 1)
        values = jnp.where(row == column, weight, 0.0) + jnp.where(row + 1 == column, 1.0 - weight, 0.0)
        high, low = split(values[:, : 8 * RECEIVED])
        w_take[pl.ds(0, LINES), :] = high
        w_take[pl.ds(LINES, LINES), :] = low

    n_early, n_relays = tab[EARLY], tab[RELAYS]

    def forward(j, q):
        at = starts["relays"] + 3 * j
        arrived(tab[at], q).wait_recv()
        copy(n_sends + j, at, q).start()

    for q in range(CHUNKS + 1):
        if q < CHUNKS:
            @pl.loop(0, n_early)
            def _(j):
                forward(j, q)
        if q > 0:
            @pl.loop(n_early, n_relays)
            def _(j):
                forward(j, q - 1)

    def pool_columns(blocks):
        rows = blocks[0].shape[0]
        high, low = split(jnp.concatenate(blocks, axis=0))
        both = mm(high, pool[...]) + mm(low, pool[...])
        return [both[rows * i : rows * i + rows] for i in range(len(blocks))]

    def halve(tiles, count, rows):
        def one(i):
            return tiles[i, pl.ds(0, rows, 2), :] + tiles[i, pl.ds(1, rows, 2), :]

        return pool_columns(
            [jnp.concatenate([one(i), one(i + 1)], axis=1) for i in range(0, count, 2)]
        )

    for q in range(CHUNKS):
        for span in (SPANS, SPANS + 2):
            @pl.loop(tab[span], tab[span + 1])
            def _(i):
                arrived(TAKEN + i, q).wait_recv()

        @pl.when(jnp.logical_not(blended))
        def _():
            for t in range(0, CHUNK, STEP):
                x = buf[q, pl.ds(TAKEN, RECEIVED), :, pl.ds(t, STEP)].reshape(8 * RECEIVED, STEP)
                x = jnp.where(lax.broadcasted_iota(jnp.int32, x.shape, 0) < 8 * n_taken, x, 0.0)
                merc[:, pl.ds(q * CHUNK + t, STEP)] = weighted(w_take[...], x)

        @pl.when(blended)
        def _():
            @pl.when(r < FIRST_KEPT)
            def _():
                merc[:, chunk(q)] = buf[q, pl.ds(TAKEN, 16)].reshape(LINES, CHUNK)

            @pl.when(r >= FIRST_KEPT)
            def _():
                for t in range(0, CHUNK, STEP):
                    x = buf[q, pl.ds(TAKEN, 16), :, pl.ds(t, STEP)].reshape(LINES, STEP)
                    x = jnp.where(lax.broadcasted_iota(jnp.int32, x.shape, 0) < 8 * tab[SPANS + 1], x, 0.0)
                    own = buf[q, pl.ds(OWN, 16), :, pl.ds(t, STEP)].reshape(LINES, STEP)
                    merc[:, pl.ds(q * CHUNK + t, STEP)] = x + weighted(w_take[:, :LINES], own)

            for i in range(most_extra):
                @pl.when(i < tab[EXTRAS])
                def _():
                    rows = pl.ds(pl.multiple_of(tab[starts["extra"] + i] * 8, 8), 8)
                    merc[rows, chunk(q)] += buf[q, TAKEN + 16 + i]

        for i in range(CHUNK // 128):
            tiles0[i] = merc[:, pl.ds(q * CHUNK + 128 * i, 128)]
        for i, part in enumerate(halve(tiles0, CHUNK // 128, 64)):
            tiles1[i] = part
            out1[:, pl.ds(q * CHUNK // 2 + 128 * i, 128)] = part
        for i, part in enumerate(halve(tiles1, CHUNK // 256, 32)):
            tiles2[i] = part
            out2[:, pl.ds(q * CHUNK // 4 + 128 * i, 128)] = part
        for i, part in enumerate(halve(tiles2, CHUNK // 512, 16)):
            for k in range(4):
                l3_send[k, :, pl.ds(q * CHUNK // 8 + 128 * i, 128)] = part[4 * k : 4 * k + 4]

    ys = []
    for k in range(1, 4):
        other = lax.rem(c + k, 4)
        ys.append(
            pltpu.make_async_remote_copy(
                src_ref=l3_send.at[other],
                dst_ref=l3_take.at[c],
                send_sem=y_send_sem.at[k - 1],
                recv_sem=y_take_sem.at[k - 1],
                device_id=(r, other),
                device_id_type=pl.DeviceIdType.MESH,
            )
        )
    for y in ys:
        y.start()
    for y in ys:
        y.wait_recv()
    for k in range(4):
        out3[:, pl.ds(k * WIDTH // 8, WIDTH // 8)] = jnp.where(c == k, l3_send[k], l3_take[k])
    level3 = out3[...]
    sums = jnp.concatenate(
        [level3[0:1] + level3[1:2], level3[2:3] + level3[3:4], jnp.zeros((6, WIDTH // 2), jnp.float32)],
        axis=0,
    )
    for i, part in enumerate(pool_columns([sums[:, 256 * i : 256 * i + 256] for i in range(16)])):
        out4[:, pl.ds(128 * i, 128)] = part[:2]

    for y in ys:
        y.wait_send()
    for q in range(CHUNKS):
        @pl.loop(0, n_own)
        def _(j):
            copy(j, starts["sends"] + 3 * j, q).wait_send()

        @pl.loop(0, n_relays)
        def _(j):
            copy(n_sends + j, starts["relays"] + 3 * j, q).wait_send()


def store(*refs):
    *arrays, sems = refs
    copies = []
    for i in range(4):
        rows = pl.ds(32 * i, 32)
        copies.append(pltpu.make_async_copy(arrays[0].at[rows], arrays[5].at[rows], sems.at[i]))
    for i in range(1, 5):
        copies.append(pltpu.make_async_copy(arrays[i], arrays[5 + i], sems.at[3 + i]))
    for copy in copies:
        copy.start()
    for copy in copies:
        copy.wait()


def body(source, low_row, weight_low):
    words, starts, size, most_passed, n_sends, n_relays = make_tables()
    slots = PASSED + most_passed
    f32 = jnp.float32
    vmem = pl.BlockSpec(memory_space=pltpu.VMEM)
    results = pl.pallas_call(
        functools.partial(kernel, words, starts, n_sends, starts["peers"] - starts["extra"]),
        out_shape=(
            jax.ShapeDtypeStruct((128, 8192), f32),
            jax.ShapeDtypeStruct((64, 4096), f32),
            jax.ShapeDtypeStruct((32, 2048), f32),
            jax.ShapeDtypeStruct((4, 4096), f32),
            jax.ShapeDtypeStruct((2, 2048), f32),
        ),
        in_specs=[pl.BlockSpec(memory_space=pl.ANY), vmem, vmem],
        out_specs=(vmem,) * 5,
        scratch_shapes=[
            pltpu.VMEM((CHUNKS, slots, 8, CHUNK), f32),
            pltpu.SMEM((size,), jnp.int32),
            pltpu.VMEM((2 * LINES, LINES), jnp.bfloat16),
            pltpu.VMEM((2 * LINES, 8 * RECEIVED), jnp.bfloat16),
            pltpu.VMEM((256, 128), jnp.bfloat16),
            pltpu.VMEM((CHUNK // 128, 128, 128), f32),
            pltpu.VMEM((CHUNK // 256, 64, 128), f32),
            pltpu.VMEM((CHUNK // 512, 32, 128), f32),
            pltpu.VMEM((4, 4, WIDTH // 8), f32),
            pltpu.VMEM((4, 4, WIDTH // 8), f32),
            pltpu.SemaphoreType.DMA((CHUNKS,)),
            pltpu.SemaphoreType.DMA((n_sends + n_relays, CHUNKS)),
            pltpu.SemaphoreType.DMA((RECEIVED + most_passed, CHUNKS)),
            pltpu.SemaphoreType.DMA((3,)),
            pltpu.SemaphoreType.DMA((3,)),
        ],
        compiler_params=pltpu.CompilerParams(
            collective_id=0, has_side_effects=True, vmem_limit_bytes=48 * 2**20
        ),
    )(source.reshape(16, 8, WIDTH), low_row.reshape(64, 128), weight_low.reshape(64, 128))
    return pl.pallas_call(
        store,
        out_shape=tuple(jax.ShapeDtypeStruct(v.shape, v.dtype) for v in results),
        in_specs=[vmem] * 5,
        out_specs=(pl.BlockSpec(memory_space=pl.ANY),) * 5,
        scratch_shapes=[pltpu.SemaphoreType.DMA((8,))],
        compiler_params=pltpu.CompilerParams(vmem_limit_bytes=2**20),
    )(*results)


def solution(mesh):
    placed = (P("rows", "cols"), P(), P())
    return jax.shard_map(
        body,
        mesh=mesh,
        in_specs=placed,
        out_specs=(
            P("rows", "cols"),
            P("rows", "cols"),
            P("rows", "cols"),
            P(("rows", "cols"), None),
            P(("rows", "cols"), None),
        ),
        check_vma=False,
    )
```
